32 devices in a mesh: head: 4 (over z), pts: 8 (over y, x, core).
Axes of the slice: x: 2, y: 2, z: 4, core: 2. Of those that a mesh axis runs over, the one named last changes fastest.
Arguments:
- layer_inputs_trainorder: bfloat16 [196608, 256], P(('head', 'pts')), may hold values from -6 to 6
- inference_placement: int32 [196608], P(('head', 'pts')), may hold values from 0 to 196607, as said below
- initial_layernorm_gain: float32 [256], replicated, may hold values from 0.1 to 1.9
- initial_layernorm_offset: float32 [256], replicated, may hold values from -2 to 2
- attribute_projection: bfloat16 [256, 256], replicated, may hold values from -0.375 to 0.375
- assignment_feeder_projection: bfloat16 [256, 256], replicated, may hold values from -0.375 to 0.375
- partition_projection: bfloat16 [16, 32], replicated, may hold values from -1.5 to 1.5
- partition_offset: float32 [32], replicated, may hold values from -4 to 4
- softmax_sharpness: float32 [16], P('head'), may hold values from 0.03 to 1
- partition_question_map: float32 [16, 16], replicated, may hold values from -1.5 to 1.5
- partition_lookup_map: float32 [16, 16], replicated, may hold values from -1.5 to 1.5
- partition_content_map: float32 [16, 16], replicated, may hold values from -1.5 to 1.5
- emitted_projection: bfloat16 [256, 256], replicated, may hold values from -0.375 to 0.375
- emitted_offset: float32 [256], replicated, may hold values from -2 to 2
- latter_layernorm_gain: float32 [256], replicated, may hold values from 0.1 to 1.9
- latter_layernorm_offset: float32 [256], replicated, may hold values from -2 to 2
- perceptron_entry_map: bfloat16 [256, 1024], replicated, may hold values from -0.375 to 0.375
- perceptron_entry_offset: float32 [1024], replicated, may hold values from -2 to 2
- perceptron_exit_map: bfloat16 [1024, 256], replicated, may hold values from -0.1875 to 0.1875
- perceptron_exit_offset: float32 [256], replicated, may hold values from -2 to 2
Outputs:
- served: bfloat16 [8, 24576, 256], P('pts', 'head')
The draws below stay inside these ranges and needn't reach their ends.
Inputs may be any that keep to these rules, and one draw needn't show every extreme that they name: inference_placement is a permutation of all points; of the 6144 points of each aligned block of the training order, exactly 192 go to each aligned block of 6144 serving positions.
All inputs are finite; a program needn't handle non-finite values.
Results may differ from the reference program's by a relative error of at most 0.0035.
The reference program's roundings to bfloat16 on the way count: a program that leaves them out, or rounds other values in their place, can miss the bound.
Values may be sent and summed in bfloat16 or wider, within the bound.
A program may use at most 128 MiB of HBM per device.

```python
import math
import jax
import jax.numpy as jnp
from jax import lax

ATTENDER_TOTAL = 16
DH = 16
M = 32
FF = 1024
PTS_DEV = 6144
MODEL_CHANNELS = 256
SERVE = 24576
POINTS = 196608
N_PTS = 8


def draw_inference_placement(key, part):
    blocks = POINTS // PTS_DEV
    per_pair = PTS_DEV // blocks
    first_keys = jax.random.split(jax.random.fold_in(key, 11), blocks)
    second_keys = jax.random.split(jax.random.fold_in(key, 12), blocks)
    within = jax.vmap(lambda single: jax.random.permutation(single, PTS_DEV))(first_keys).astype(jnp.int32)
    arrival = jax.vmap(lambda single: jax.random.permutation(single, PTS_DEV))(second_keys).astype(jnp.int32)
    target = within // per_pair
    ranks_in = within % per_pair
    source_ids = jnp.arange(blocks, dtype=jnp.int32)[:, None]
    slot_ids = source_ids * per_pair + ranks_in
    positions = target * PTS_DEV + arrival[target, slot_ids]
    return positions.reshape(-1).astype(jnp.int32)


def level_of(key, shape, cuts, smallest, high):
    loudness, own = 1.0, jax.random.fold_in(key, 6)
    for axis_at, parts in cuts:
        steps = jnp.exp(jax.random.uniform(jax.random.fold_in(own, axis_at), (parts,), jnp.float32, smallest / len(cuts), high / len(cuts)))
        loudness = loudness * jnp.repeat(steps, shape[axis_at] // parts).reshape([-1 if axis == axis_at else 1 for axis in range(len(shape))])
    return loudness


def bell_draw(stream_key, shape, deviation, bound, cuts=(), held_as=jnp.bfloat16):
    loudness = level_of(stream_key, shape, cuts, -0.22, 0.18) if cuts else 1.0
    result = jax.random.normal(stream_key, shape, jnp.float32) * deviation * loudness
    return jnp.minimum(jnp.maximum(result, -bound), bound).astype(held_as)


def setup_inputs(seed: int = 0) -> dict:
    key_of = jax.random.split(jax.random.key(seed), 21)
    return {
        "layer_inputs_trainorder": bell_draw(key_of[0], (POINTS, MODEL_CHANNELS), 1.0, 6.0, ((0, 32),)),
        "inference_placement": draw_inference_placement(jax.random.fold_in(key_of[20], 71), 0),
        "initial_layernorm_gain": jnp.clip(1.0 + 0.18 * jax.random.normal(key_of[2], (MODEL_CHANNELS,), jnp.float32), 0.1, 1.9),
        "initial_layernorm_offset": bell_draw(key_of[3], (MODEL_CHANNELS,), 0.3, 2.0, (), jnp.float32),
        "attribute_projection": bell_draw(key_of[4], (MODEL_CHANNELS, MODEL_CHANNELS), MODEL_CHANNELS ** -0.5, 0.375),
        "assignment_feeder_projection": bell_draw(key_of[5], (MODEL_CHANNELS, MODEL_CHANNELS), MODEL_CHANNELS ** -0.5, 0.375),
        "partition_projection": bell_draw(key_of[6], (DH, M), DH ** -0.5, 1.5),
        "partition_offset": bell_draw(key_of[7], (M,), 1.0, 4.0, (), jnp.float32),
        "softmax_sharpness": jnp.clip(jnp.exp(math.log(1.0) - 3.506558 * jax.random.uniform(key_of[8], (ATTENDER_TOTAL,), jnp.float32) ** level_of(key_of[8], (ATTENDER_TOTAL,), ((0, 4),), -0.2, 0.2)), 0.03, 1.0),
        "partition_question_map": bell_draw(key_of[9], (DH, DH), DH ** -0.5, 1.5, (), jnp.float32),
        "partition_lookup_map": bell_draw(key_of[10], (DH, DH), DH ** -0.5, 1.5, (), jnp.float32),
        "partition_content_map": bell_draw(key_of[11], (DH, DH), DH ** -0.5, 1.5, (), jnp.float32),
        "emitted_projection": bell_draw(key_of[12], (MODEL_CHANNELS, MODEL_CHANNELS), MODEL_CHANNELS ** -0.5, 0.375),
        "emitted_offset": bell_draw(key_of[13], (MODEL_CHANNELS,), 0.3, 2.0, (), jnp.float32),
        "latter_layernorm_gain": jnp.clip(1.0 + 0.18 * jax.random.normal(key_of[14], (MODEL_CHANNELS,), jnp.float32), 0.1, 1.9),
        "latter_layernorm_offset": bell_draw(key_of[15], (MODEL_CHANNELS,), 0.3, 2.0, (), jnp.float32),
        "perceptron_entry_map": bell_draw(key_of[16], (MODEL_CHANNELS, FF), MODEL_CHANNELS ** -0.5, 0.375),
        "perceptron_entry_offset": bell_draw(key_of[17], (FF,), 0.3, 2.0, (), jnp.float32),
        "perceptron_exit_map": bell_draw(key_of[18], (FF, MODEL_CHANNELS), FF ** -0.5, 0.1875),
        "perceptron_exit_offset": bell_draw(key_of[19], (MODEL_CHANNELS,), 0.3, 2.0, (), jnp.float32),
    }


def layer_norm(row_block, gain_vec, bias_vec):
    row_mean = lax.optimization_barrier(jnp.mean(row_block, axis=-1, keepdims=True))
    centred = row_block - row_mean
    spread = lax.optimization_barrier(jnp.mean(centred * centred, axis=-1, keepdims=True))
    return centred * lax.rsqrt(spread + 1e-05) * gain_vec + bias_vec

def truncated_coefficients(value):
    return lax.optimization_barrier(value.astype(jnp.bfloat16)).astype(jnp.float32)

def partition_share_entries(standardized_entries, assignment_feeder_projection, partition_projection, partition_offset, softmax_sharpness):
    middle = truncated_coefficients(jnp.dot(standardized_entries, assignment_feeder_projection, preferred_element_type=jnp.float32)).reshape(-1, ATTENDER_TOTAL, DH)
    partition_scores_raw = jnp.einsum('rhd,dm->rhm', middle, partition_projection.astype(jnp.float32))
    partition_scores_raw = (partition_scores_raw + partition_offset) / softmax_sharpness[:, None]
    return jax.nn.softmax(partition_scores_raw, axis=-1)

def reference(layer_inputs_trainorder, inference_placement, initial_layernorm_gain, initial_layernorm_offset, attribute_projection, assignment_feeder_projection, partition_projection, partition_offset, softmax_sharpness, partition_question_map, partition_lookup_map, partition_content_map, emitted_projection, emitted_offset, latter_layernorm_gain, latter_layernorm_offset, perceptron_entry_map, perceptron_entry_offset, perceptron_exit_map, perceptron_exit_offset):
    block_count = POINTS // PTS_DEV
    row_blocks = layer_inputs_trainorder.reshape(block_count, PTS_DEV, MODEL_CHANNELS)

    def gather_sums(running_state, row_block):
        standardized_entries = layer_norm(row_block.astype(jnp.float32), initial_layernorm_gain, initial_layernorm_offset).astype(jnp.bfloat16)
        slice_feature_rows = truncated_coefficients(jnp.dot(standardized_entries, attribute_projection, preferred_element_type=jnp.float32)).reshape(-1, ATTENDER_TOTAL, DH)
        coefficient_array = partition_share_entries(standardized_entries, assignment_feeder_projection, partition_projection, partition_offset, softmax_sharpness)
        coefficients_halfprecision = truncated_coefficients(coefficient_array)
        return ((running_state[0] + lax.optimization_barrier(jnp.sum(coefficient_array, axis=0)), running_state[1] + jnp.einsum('qct,qcv->ctv', coefficients_halfprecision, slice_feature_rows)), None)
    start = (jnp.zeros((ATTENDER_TOTAL, M), jnp.float32), jnp.zeros((ATTENDER_TOTAL, M, DH), jnp.float32))
    (totals, numerator), unused = lax.scan(gather_sums, start, row_blocks)
    slice_token = numerator / (totals + 1e-05)[:, :, None]
    highest_mode = lax.Precision.HIGHEST
    query_rows = jnp.einsum('izn,nu->izu', slice_token, partition_question_map, precision=highest_mode)
    key_vectors = jnp.einsum('izn,nu->izu', slice_token, partition_lookup_map, precision=highest_mode)
    value_rows = jnp.einsum('izn,nu->izu', slice_token, partition_content_map, precision=highest_mode)
    score_scale = 1.0 / math.sqrt(DH)
    scores = jnp.einsum('hme,hne->hmn', query_rows, key_vectors, precision=highest_mode) * score_scale
    attention = jax.nn.softmax(scores, axis=-1)
    slice_output = truncated_coefficients(jnp.einsum('hmn,hne->hme', attention, value_rows, precision=highest_mode))
    inverse = jnp.argsort(inference_placement).astype(jnp.int32).reshape(block_count, PTS_DEV)

    def serve_block(serve_index):
        row_block = jnp.take(layer_inputs_trainorder, serve_index, axis=0)
        standardized_entries = layer_norm(row_block.astype(jnp.float32), initial_layernorm_gain, initial_layernorm_offset).astype(jnp.bfloat16)
        coefficients_halfprecision = truncated_coefficients(partition_share_entries(standardized_entries, assignment_feeder_projection, partition_projection, partition_offset, softmax_sharpness))
        blended_rows = jnp.einsum('fny,nyp->fnp', coefficients_halfprecision, slice_output).astype(jnp.bfloat16).reshape(-1, MODEL_CHANNELS)
        hidden = row_block.astype(jnp.float32) + jnp.dot(blended_rows, emitted_projection, preferred_element_type=jnp.float32) + emitted_offset
        normed_two = layer_norm(hidden, latter_layernorm_gain, latter_layernorm_offset).astype(jnp.bfloat16)
        inner_act = jax.nn.gelu(jnp.dot(normed_two, perceptron_entry_map, preferred_element_type=jnp.float32) + perceptron_entry_offset, approximate=False).astype(jnp.bfloat16)
        return (hidden + jnp.dot(inner_act, perceptron_exit_map, preferred_element_type=jnp.float32) + perceptron_exit_offset).astype(jnp.bfloat16)
    served = lax.map(serve_block, inverse)
    return served.reshape(N_PTS, SERVE, MODEL_CHANNELS)
```

```python
import functools
import math

import jax
import jax.numpy as jnp
from jax import lax
from jax.experimental import pallas as pl
from jax.experimental.pallas import tpu as pltpu
from jax.sharding import PartitionSpec as P

DH = 16
LANES = 128
STEPS = 16
EARLY = 12
F32 = jnp.float32
BF16 = jnp.bfloat16
I32 = jnp.int32
HIGHEST = lax.Precision.HIGHEST
LOG2E = math.log2(math.e)
NT = (((1,), (1,)), ((), ()))
MESH = pl.DeviceIdType.MESH


def norm_rows(rows, gain, bias):
    mean = jnp.mean(rows, axis=-1, keepdims=True)
    centred = rows - mean
    spread = jnp.mean(centred * centred, axis=-1, keepdims=True)
    return (centred * lax.rsqrt(spread + 1e-05) * gain + bias).astype(BF16)


def slice_weights(feeder_t, expand, offset, scale, slices):
    raw = jnp.dot(expand, feeder_t, preferred_element_type=F32)
    logit = (raw + offset) * scale
    lanes = logit.shape[1]
    logit = logit.reshape(-1, slices, lanes)
    powers = jnp.exp2(logit - jnp.max(logit, axis=1, keepdims=True))
    share = powers * (1.0 / jnp.sum(powers, axis=1, keepdims=True))
    return share.reshape(-1, lanes)


def same_head(shape, row_size, column_size):
    row_head = lax.broadcasted_iota(I32, shape, 0) // row_size
    column_head = lax.broadcasted_iota(I32, shape, 1) // column_size
    return row_head == column_head


def exact_gelu(h):
    half = 0.5 * h
    return half + half * lax.erf(h * (1.0 / math.sqrt(2.0)))


def floor_div(value, divisor):
    return ((value.astype(F32) + 0.5) * (1.0 / divisor)).astype(I32)


def flip(a, b, size):
    result, bit = 0, 1
    while bit < size:
        result = result + (a // bit + b // bit) % 2 * bit
        bit *= 2
    return result


def index_kernel(groups, shards, rows, place_ref, order_ref, spots_ref, rank_v, target_v, spot_v):
    devices = groups * shards
    chunks = rows // LANES

    place = place_ref[...]
    block = floor_div(place, rows)
    shard = floor_div(block, groups)
    target = (block - shard * groups) * shards + shard
    target_v[...] = target
    spot_v[...] = place - block * rows
    upper = (
        lax.broadcasted_iota(I32, (LANES, LANES), 0) <= lax.broadcasted_iota(I32, (LANES, LANES), 1)
    ).astype(F32).astype(BF16)
    stacked = jnp.concatenate(
        [
            (lax.broadcasted_iota(I32, (devices, LANES), 0)
             == target[:, at * LANES : (at + 1) * LANES]).astype(F32)
            for at in range(chunks)
        ],
        axis=0,
    )
    prefix = jnp.dot(stacked.astype(BF16), upper, preferred_element_type=F32)
    run = jnp.zeros((devices, 1), F32)
    for at in range(chunks):
        span = slice(at * devices, (at + 1) * devices)
        ahead = jnp.sum(stacked[span] * (prefix[span] + (run - 1.0)), axis=0, keepdims=True)
        rank_v[:, at * LANES : (at + 1) * LANES] = ahead.astype(I32)
        run = run + prefix[span][:, LANES - 1 :]

    wide = order_ref.shape[1]
    part_lanes = 4 * LANES

    def invert(at, total_so_far):
        lanes = pl.ds(pl.multiple_of(at * part_lanes, part_lanes), part_lanes)
        hot = (
            lax.broadcasted_iota(I32, (devices, part_lanes), 0) == target_v[:, lanes]
        ).astype(F32)
        slot_hot = (
            lax.broadcasted_iota(I32, (wide, part_lanes), 0) == rank_v[:, lanes]
        ).astype(F32).astype(BF16)
        index = lax.broadcasted_iota(I32, (1, part_lanes), 1) + at * part_lanes
        values = []
        for value in (index, spot_v[:, lanes]):
            high = value // 64
            values += [hot * high.astype(F32), hot * (value - high * 64).astype(F32)]
        values = jnp.concatenate(values, axis=0).astype(BF16)
        return total_so_far + lax.dot_general(values, slot_hot, NT, preferred_element_type=F32)

    table = lax.fori_loop(
        0, rows // part_lanes, invert, jnp.zeros((4 * devices, wide), F32)
    )
    order_ref[...] = (table[:devices] * 64.0 + table[devices : 2 * devices]).astype(I32)
    spots = table[2 * devices : 3 * devices] * 64.0 + table[3 * devices :]
    for at in range(devices):
        spots_ref[at] = spots[at : at + 1].astype(I32)


def fused_kernel(
    slices, groups, shards,
    x_hbm, order_s, meta_v, sharp_ref, gain_ref, bias_ref, attribute_ref, feeder_ref, project_ref,
    offset_row_ref, question_ref, lookup_ref, content_ref, emit_ref, emit_bias_ref,
    gain2_ref, bias2_ref, entry_ref, entry_bias_ref, exit_ref, exit_bias_ref,
    res_hbm, meta_in,
    x_v, xf, stage, send_v, recv_v, res,
    sharp_v, sharp_in, w_ref, expand_ref, offset_ref, scale_ref, numer, total,
    part_out, part_in, mine, all_in, sums_v, blend,
    local_sem, out_sem, row_send, row_recv, meta_send, meta_recv, sharp_send, sharp_recv,
    part_send, part_recv, all_send, all_recv,
):
    devices = groups * shards
    rows, width = x_v.shape
    per_pair = rows // devices
    tile = rows // STEPS
    blocks = devices // STEPS
    columns = expand_ref.shape[0]
    own = sharp_ref.shape[1]
    my_head, my_pts = lax.axis_index("head"), lax.axis_index("pts")
    me = my_head * shards + my_pts

    def peer(slot):
        return flip(my_head, slot % groups, groups), flip(my_pts, slot // groups, shards)

    def flat(slot):
        head, pts = peer(slot)
        return head * shards + pts

    def loop(low, high, step):
        def run(at, carry):
            step(at)
            return carry
        lax.fori_loop(low, high, run, 0)

    barrier = pltpu.get_barrier_semaphore()
    loop(1, devices, lambda slot: pl.semaphore_signal(
        barrier, 1, device_id=peer(slot), device_id_type=MESH
    ))
    load = pltpu.make_async_copy(x_hbm, x_v, local_sem.at[0])
    load.start()

    sharp_v[...] = jnp.zeros_like(sharp_v)
    sharp_v[:, :own] = sharp_ref[...]
    sharp_in[my_head] = sharp_v[...]

    w_ref[:width] = attribute_ref[...].astype(F32).T.astype(BF16)
    w_ref[width:] = feeder_ref[...].astype(F32).T.astype(BF16)
    repeated = jnp.concatenate([project_ref[...].astype(F32).T] * (columns // slices), axis=0)
    lane = lax.broadcasted_iota(I32, (DH, width), 1) % DH
    pick = (lane == lax.broadcasted_iota(I32, (DH, width), 0)).astype(F32).astype(BF16)
    filled = jnp.dot(repeated.astype(BF16), pick, preferred_element_type=F32)
    expand_ref[...] = jnp.where(same_head(filled.shape, slices, DH), filled, 0.0).astype(BF16)
    row = lax.broadcasted_iota(I32, (columns, slices), 0) % slices
    match = row == lax.broadcasted_iota(I32, (columns, slices), 1)
    offset_ref[...] = jnp.sum(jnp.where(match, offset_row_ref[...], 0.0), axis=1, keepdims=True)
    numer[...] = jnp.zeros_like(numer)
    total[...] = jnp.zeros_like(total)

    pl.semaphore_wait(barrier, devices - 1)

    def sharp_copy(step):
        return pltpu.make_async_remote_copy(
            sharp_v, sharp_in.at[my_head], sharp_send.at[step], sharp_recv.at[step],
            device_id=(flip(my_head, step, groups), my_pts), device_id_type=MESH,
        )

    def meta_copy(slot):
        return pltpu.make_async_remote_copy(
            meta_v.at[flat(slot)], meta_in.at[slot], meta_send.at[slot], meta_recv.at[slot],
            device_id=peer(slot), device_id_type=MESH,
        )

    def row_copy(slot):
        span = pl.ds(pl.multiple_of(slot * per_pair, per_pair), per_pair)
        return pltpu.make_async_remote_copy(
            send_v.at[span], recv_v.at[span], row_send.at[slot], row_recv.at[slot],
            device_id=peer(slot), device_id_type=MESH,
        )

    def part_copy(slot):
        return pltpu.make_async_remote_copy(
            part_out.at[flat(slot)], part_in.at[slot], part_send.at[slot], part_recv.at[slot],
            device_id=peer(slot), device_id_type=MESH,
        )

    def all_copy(slot):
        return pltpu.make_async_remote_copy(
            mine, all_in.at[me], all_send.at[slot], all_recv.at[slot],
            device_id=peer(slot), device_id_type=MESH,
        )

    loop(1, groups, lambda step: sharp_copy(step).start())
    loop(1, devices, lambda slot: meta_copy(slot).start())
    meta_in[0] = meta_v[me]

    load.wait()

    def widen(at):
        part = x_v[pl.ds(pl.multiple_of(at * tile, tile), tile), :].astype(F32)
        xf[pl.ds(at * 2 * tile, tile, stride=2), :] = part[:, :LANES]
        xf[pl.ds(at * 2 * tile + 1, tile, stride=2), :] = part[:, LANES:]

    loop(0, STEPS, widen)
    loop(1, groups, lambda step: sharp_copy(step).wait())
    per_group = own * slices
    for group in range(groups):
        lane = lax.broadcasted_iota(I32, (per_group, LANES), 1)
        member = lax.broadcasted_iota(I32, (per_group, LANES), 0) // slices
        sharp = jnp.sum(jnp.where(lane == member, sharp_in[group], 0.0), axis=1, keepdims=True)
        scale_ref[group * per_group : (group + 1) * per_group] = LOG2E / sharp

    def sums_step(at):
        @pl.when(jnp.logical_and(at > 0, at <= EARLY // blocks))
        def _():
            for way in range(blocks):
                slot = (at - 1) * blocks + way

                @pl.when(slot > 0)
                def _():
                    row_copy(slot).start()

        for way in range(blocks):
            goal = flat(at * blocks + way)
            for k in range(per_pair):
                put = 2 * (way * per_pair + k)
                stage[put : put + 2, :] = xf[pl.ds(order_s[goal, k] * 2, 2), :]
        span = pl.ds(pl.multiple_of(at * tile, tile), tile)
        send_v[span, :LANES] = stage[pl.ds(0, tile, stride=2), :].astype(BF16)
        send_v[span, LANES:] = stage[pl.ds(1, tile, stride=2), :].astype(BF16)

        normed = norm_rows(x_v[span, :].astype(F32), gain_ref[...], bias_ref[...])
        both = lax.dot_general(w_ref[...], normed, NT, preferred_element_type=F32).astype(BF16)
        share = slice_weights(
            both[width:], expand_ref[...], offset_ref[...], scale_ref[...], slices
        )
        numer[...] += lax.dot_general(
            both[:width], share.astype(BF16), NT, preferred_element_type=F32
        )
        part = share[:, :LANES]
        for low in range(LANES, tile, LANES):
            part += share[:, low : low + LANES]
        total[...] += part

    loop(0, STEPS, sums_step)

    kept = jnp.where(same_head(numer.shape, DH, slices), numer[...], 0.0)
    sums_v[:DH] = jnp.sum(kept.reshape(-1, DH, columns), axis=0)
    sums_v[DH:] = lax.dot_general(
        jnp.ones((8, LANES), F32), total[...], NT, precision=HIGHEST, preferred_element_type=F32
    )
    per_row = columns // LANES
    depth = part_out.shape[1]
    places = [
        (at // per_row, at % per_row * LANES, at // depth, at % depth)
        for at in range((DH + 1) * per_row)
    ]
    part_out[...] = jnp.zeros_like(part_out)
    for line, low, piece, inner in places:
        part_out[piece, inner : inner + 1, :] = sums_v[line : line + 1, low : low + LANES]
    loop(1, devices, lambda slot: part_copy(slot).start())
    part_in[0] = part_out[me]
    loop(max(EARLY, 1), devices, lambda slot: row_copy(slot).start())

    loop(1, devices, lambda slot: part_copy(slot).wait())
    mine[...] = jnp.sum(part_in[...], axis=0)
    loop(1, devices, lambda slot: all_copy(slot).start())
    all_in[me] = mine[...]
    loop(1, devices, lambda slot: all_copy(slot).wait())
    for line, low, piece, inner in places:
        sums_v[line : line + 1, low : low + LANES] = all_in[piece, inner : inner + 1, :]

    stok = sums_v[:DH] / (sums_v[DH : DH + 1] + 1e-05)
    query, key, value = (
        jnp.dot(m[...].T, stok, precision=HIGHEST, preferred_element_type=F32)
        for m in (question_ref, lookup_ref, content_ref)
    )
    scores = jnp.dot(key.T, query, precision=HIGHEST, preferred_element_type=F32)
    scores = scores * (1.0 / math.sqrt(DH))
    mask = same_head(scores.shape, slices, slices)
    scores = jnp.where(mask, scores, -jnp.inf)
    powers = jnp.exp(scores - jnp.max(scores, axis=0, keepdims=True))
    attention = powers / jnp.sum(powers, axis=0, keepdims=True)
    sout = jnp.dot(value, attention, precision=HIGHEST, preferred_element_type=F32)
    spread = jnp.concatenate([sout] * (width // DH), axis=0)
    blend[...] = jnp.where(same_head(blend.shape, DH, slices), spread, 0.0).astype(BF16)
    recv_v[:per_pair] = send_v[:per_pair]

    def rows_step(at):
        def arrived(way):
            slot = at * blocks + way

            @pl.when(slot > 0)
            def _():
                row_copy(slot).wait_recv()

        loop(0, blocks, arrived)
        x = recv_v[pl.ds(pl.multiple_of(at * tile, tile), tile), :].astype(F32)
        normed = norm_rows(x, gain_ref[...], bias_ref[...])
        feeder = lax.dot_general(
            w_ref[width:], normed, NT, preferred_element_type=F32
        ).astype(BF16)
        share = slice_weights(feeder, expand_ref[...], offset_ref[...], scale_ref[...], slices)
        mixed = jnp.dot(blend[...], share.astype(BF16), preferred_element_type=F32)
        y = (
            x
            + jnp.dot(mixed.T.astype(BF16), emit_ref[...], preferred_element_type=F32)
            + emit_bias_ref[...]
        )
        z = norm_rows(y, gain2_ref[...], bias2_ref[...])
        result = y + exit_bias_ref[...]
        for low in range(0, entry_ref.shape[1], width):
            h = jnp.dot(z, entry_ref[:, low : low + width], preferred_element_type=F32)
            g = exact_gelu(h + entry_bias_ref[:, low : low + width]).astype(BF16)
            result += jnp.dot(g, exit_ref[low : low + width], preferred_element_type=F32)
        res[pl.ds(at * 2 * tile, tile, stride=2), :] = result[:, :LANES]
        res[pl.ds(at * 2 * tile + 1, tile, stride=2), :] = result[:, LANES:]
        out_copy(at).start()

    def out_copy(at):
        span = pl.ds(pl.multiple_of(at * 2 * tile, 2 * tile), 2 * tile)
        return pltpu.make_async_copy(res.at[span], res_hbm.at[span], out_sem.at[at])

    loop(0, STEPS, rows_step)
    loop(1, devices, lambda slot: meta_copy(slot).wait())
    loop(1, devices, lambda slot: row_copy(slot).wait_send())
    loop(0, STEPS, lambda at: out_copy(at).wait())


def serve_kernel(spot_s, res_ref, out_ref, placed):
    step = pl.program_id(0)
    tile = res_ref.shape[0] // 2
    blocks = spot_s.shape[0] // pl.num_programs(0)
    per_pair = tile // blocks
    for way in range(blocks):
        for k in range(per_pair):
            spot = spot_s[step * blocks + way, 0, k]
            at = 2 * (way * per_pair + k)
            placed[pl.ds(pl.multiple_of(spot * 2, 2), 2), :] = res_ref[at : at + 2, :]

    @pl.when(step == pl.num_programs(0) - 1)
    def _():
        def narrow(at, carry):
            span = pl.ds(pl.multiple_of(at * tile, tile), tile)
            out_ref[span, :LANES] = placed[pl.ds(at * 2 * tile, tile, stride=2), :].astype(BF16)
            out_ref[span, LANES:] = placed[pl.ds(at * 2 * tile + 1, tile, stride=2), :].astype(
                BF16
            )
            return carry
        lax.fori_loop(0, out_ref.shape[0] // tile, narrow, 0)


def body(
    layer_inputs_trainorder,
    inference_placement,
    initial_layernorm_gain,
    initial_layernorm_offset,
    attribute_projection,
    assignment_feeder_projection,
    partition_projection,
    partition_offset,
    softmax_sharpness,
    partition_question_map,
    partition_lookup_map,
    partition_content_map,
    emitted_projection,
    emitted_offset,
    latter_layernorm_gain,
    latter_layernorm_offset,
    perceptron_entry_map,
    perceptron_entry_offset,
    perceptron_exit_map,
    perceptron_exit_offset,
):
    groups = lax.axis_size("head")
    shards = lax.axis_size("pts")
    devices = groups * shards
    rows, width = layer_inputs_trainorder.shape
    per_pair = rows // devices
    slices = partition_projection.shape[1]
    columns = softmax_sharpness.shape[0] * groups * slices
    wide = -(-per_pair // LANES) * LANES
    tile = rows // STEPS
    depth = -(-(DH + 1) * (columns // LANES) // devices)
    order, spots = pl.pallas_call(
        functools.partial(index_kernel, groups, shards, rows),
        out_shape=(
            jax.ShapeDtypeStruct((devices, wide), I32),
            jax.ShapeDtypeStruct((devices, 1, wide), I32),
        ),
        scratch_shapes=[pltpu.VMEM((1, rows), I32)] * 3,
    )(inference_placement[None])
    operands = (
        order, spots, softmax_sharpness[None], initial_layernorm_gain[None],
        initial_layernorm_offset[None], attribute_projection, assignment_feeder_projection,
        partition_projection, partition_offset[None], partition_question_map,
        partition_lookup_map, partition_content_map, emitted_projection, emitted_offset[None],
        latter_layernorm_gain[None], latter_layernorm_offset[None], perceptron_entry_map,
        perceptron_entry_offset[None], perceptron_exit_map, perceptron_exit_offset[None],
    )
    dma = pltpu.SemaphoreType.DMA
    scratch = [
        pltpu.VMEM((rows, width), BF16),
        pltpu.VMEM((2 * rows, LANES), F32),
        pltpu.VMEM((2 * tile, LANES), F32),
        pltpu.VMEM((rows, width), BF16),
        pltpu.VMEM((rows, width), BF16),
        pltpu.VMEM((2 * rows, LANES), F32),
        pltpu.VMEM((1, LANES), F32),
        pltpu.VMEM((groups, 1, LANES), F32),
        pltpu.VMEM((2 * width, width), BF16),
        pltpu.VMEM((columns, width), BF16),
        pltpu.VMEM((columns, 1), F32),
        pltpu.VMEM((columns, 1), F32),
        pltpu.VMEM((width, columns), F32),
        pltpu.VMEM((columns, LANES), F32),
        pltpu.VMEM((devices, depth, LANES), F32),
        pltpu.VMEM((devices, depth, LANES), F32),
        pltpu.VMEM((depth, LANES), F32),
        pltpu.VMEM((devices, depth, LANES), F32),
        pltpu.VMEM((DH + 8, columns), F32),
        pltpu.VMEM((width, columns), BF16),
        dma((2,)),
        dma((STEPS,)),
        dma((devices,)),
        dma((devices,)),
        dma((devices,)),
        dma((devices,)),
        dma((groups,)),
        dma((groups,)),
        dma((devices,)),
        dma((devices,)),
        dma((devices,)),
        dma((devices,)),
    ]
    in_vmem = pl.BlockSpec(memory_space=pltpu.VMEM)
    res, arrived = pl.pallas_call(
        functools.partial(fused_kernel, slices, groups, shards),
        out_shape=(
            jax.ShapeDtypeStruct((2 * rows, LANES), F32),
            jax.ShapeDtypeStruct((devices, 1, wide), I32),
        ),
        in_specs=[pl.BlockSpec(memory_space=pl.ANY), pl.BlockSpec(memory_space=pltpu.SMEM)]
        + [in_vmem] * (len(operands) - 1),
        out_specs=(pl.BlockSpec(memory_space=pl.ANY), in_vmem),
        scratch_shapes=scratch,
        compiler_params=pltpu.CompilerParams(
            collective_id=0, has_side_effects=True, vmem_limit_bytes=60 * 2**20
        ),
        cost_estimate=pl.CostEstimate(
            flops=rows * width * columns * 24, bytes_accessed=rows * width * 8,
            transcendentals=rows * columns * 4,
        ),
    )(layer_inputs_trainorder, *operands)
    out = pl.pallas_call(
        serve_kernel,
        grid=(STEPS,),
        in_specs=[
            pl.BlockSpec(memory_space=pltpu.SMEM),
            pl.BlockSpec((2 * tile, LANES), lambda i: (i, 0)),
        ],
        out_specs=pl.BlockSpec((rows, width), lambda i: (0, 0)),
        out_shape=jax.ShapeDtypeStruct((rows, width), BF16),
        scratch_shapes=[pltpu.VMEM((2 * rows, LANES), F32)],
        compiler_params=pltpu.CompilerParams(dimension_semantics=("arbitrary",)),
    )(arrived, res)
    return out[None]


def solution(mesh):
    placed = (
        P(("head", "pts"), None),
        P(("head", "pts")),
        P(),
        P(),
        P(),
        P(),
        P(),
        P(),
        P("head"),
        P(),
        P(),
        P(),
        P(),
        P(),
        P(),
        P(),
        P(),
        P(),
        P(),
        P(),
    )
    return jax.shard_map(
        body, mesh=mesh, in_specs=placed, out_specs=P("pts", "head", None), check_vma=False
    )
```

```python
import functools
import math

import jax
import jax.numpy as jnp
from jax import lax
from jax.experimental import pallas as pl
from jax.experimental.pallas import tpu as pltpu
from jax.sharding import PartitionSpec as P

DH = 16
LANES = 128
STEPS = 16
UNITS = 32
FIRST = 8
EARLY = 14
MID = 3
AHEAD = (4, 7)
F32 = jnp.float32
BF16 = jnp.bfloat16
I32 = jnp.int32
HIGHEST = lax.Precision.HIGHEST
LOG2E = math.log2(math.e)
NT = (((1,), (1,)), ((), ()))
MESH = pl.DeviceIdType.MESH


def norm_rows(rows, gain, bias):
    mean = jnp.mean(rows, axis=-1, keepdims=True)
    centred = rows - mean
    spread = jnp.mean(centred * centred, axis=-1, keepdims=True)
    return (centred * lax.rsqrt(spread + 1e-05) * gain + bias).astype(BF16)


def slice_weights(feeder_t, expand, offset, scale, slices):
    raw = jnp.dot(expand, feeder_t, preferred_element_type=F32)
    logit = (raw + offset) * scale
    lanes = logit.shape[1]
    logit = logit.reshape(-1, slices, lanes)
    powers = jnp.exp2(logit - jnp.max(logit, axis=1, keepdims=True))
    share = powers * (1.0 / jnp.sum(powers, axis=1, keepdims=True))
    return share.reshape(-1, lanes)


def same_head(shape, row_size, column_size):
    row_head = lax.broadcasted_iota(I32, shape, 0) // row_size
    column_head = lax.broadcasted_iota(I32, shape, 1) // column_size
    return row_head == column_head


def exact_gelu(h):
    half = 0.5 * h
    return half + half * lax.erf(h * (1.0 / math.sqrt(2.0)))


def floor_div(value, divisor):
    return ((value.astype(F32) + 0.5) * (1.0 / divisor)).astype(I32)


def flip(a, b, size):
    result, bit = 0, 1
    while bit < size:
        result = result + lax.rem(lax.div(a, bit) + lax.div(b, bit), 2) * bit
        bit *= 2
    return result


def mirror(a, size):
    result, low, high = 0, 1, size // 2
    while high >= 1:
        if isinstance(a, int):
            result = result + a // low % 2 * high
        else:
            result = result + lax.rem(lax.div(a, low), 2) * high
        low, high = low * 2, high // 2
    return result


def index_kernel(groups, shards, rows, place_ref, order_ref, spots_ref, rank_v, target_v, spot_v):
    devices = groups * shards
    chunks = rows // LANES

    place = place_ref[...]
    block = floor_div(place, rows)
    shard = floor_div(block, groups)
    apart = (block - shard * groups) ^ lax.axis_index("head")
    shard = shard ^ lax.axis_index("pts")
    bits = shards.bit_length() - 1
    shard = sum(((shard >> at) & 1) << (bits - 1 - at) for at in range(bits))
    target = shard * groups + apart
    target_v[...] = target
    spot_v[...] = place - block * rows
    upper = (
        lax.broadcasted_iota(I32, (LANES, LANES), 0) <= lax.broadcasted_iota(I32, (LANES, LANES), 1)
    ).astype(F32).astype(BF16)
    stacked = jnp.concatenate(
        [
            (lax.broadcasted_iota(I32, (devices, LANES), 0)
             == target[:, at * LANES : (at + 1) * LANES]).astype(F32)
            for at in range(chunks)
        ],
        axis=0,
    )
    prefix = jnp.dot(stacked.astype(BF16), upper, preferred_element_type=F32)
    run = jnp.zeros((devices, 1), F32)
    for at in range(chunks):
        span = slice(at * devices, (at + 1) * devices)
        ahead = jnp.sum(stacked[span] * (prefix[span] + (run - 1.0)), axis=0, keepdims=True)
        rank_v[:, at * LANES : (at + 1) * LANES] = ahead.astype(I32)
        run = run + prefix[span][:, LANES - 1 :]

    wide = order_ref.shape[1]
    part_lanes = 4 * LANES

    def invert(at, total_so_far):
        lanes = pl.ds(pl.multiple_of(at * part_lanes, part_lanes), part_lanes)
        hot = (
            lax.broadcasted_iota(I32, (devices, part_lanes), 0) == target_v[:, lanes]
        ).astype(F32)
        slot_hot = (
            lax.broadcasted_iota(I32, (wide, part_lanes), 0) == rank_v[:, lanes]
        ).astype(F32).astype(BF16)
        index = lax.broadcasted_iota(I32, (1, part_lanes), 1) + at * part_lanes
        values = []
        for value in (index, spot_v[:, lanes]):
            high = value // 64
            values += [hot * high.astype(F32), hot * (value - high * 64).astype(F32)]
        values = jnp.concatenate(values, axis=0).astype(BF16)
        return total_so_far + lax.dot_general(values, slot_hot, NT, preferred_element_type=F32)

    table = lax.fori_loop(
        0, rows // part_lanes, invert, jnp.zeros((4 * devices, wide), F32)
    )
    order_ref[...] = (table[:devices] * 64.0 + table[devices : 2 * devices]).astype(I32)
    spots = table[2 * devices : 3 * devices] * 64.0 + table[3 * devices :]
    for at in range(devices):
        spots_ref[at] = spots[at : at + 1].astype(I32)


def fused_kernel(
    slices, groups, shards,
    x_hbm, order_s, meta_v, sharp_ref, gain_ref, bias_ref, attribute_ref, feeder_ref, project_ref,
    offset_row_ref, question_ref, lookup_ref, content_ref, emit_ref, emit_bias_ref,
    gain2_ref, bias2_ref, entry_bias_ref, exit_bias_ref, entry_hbm, exit_hbm,
    res_hbm, meta_in,
    x_v, xf, stage, send_v, recv_v, res, share_v, entry_ref, exit_ref,
    sharp_v, sharp_in, w_ref, expand_ref, offset_ref, scale_ref, numer, total,
    part_out, part_in, mine, all_in, sums_v, blend,
    local_sem, out_sem, row_send, row_recv, meta_send, meta_recv, sharp_send, sharp_recv,
    part_send, part_recv, all_send, all_recv,
):
    devices = groups * shards
    rows, width = x_v.shape
    per_pair = rows // devices
    tile = rows // STEPS
    blocks = devices // STEPS
    columns = expand_ref.shape[0]
    own = sharp_ref.shape[1]
    my_head, my_pts = lax.axis_index("head"), lax.axis_index("pts")
    me = my_head * shards + my_pts

    unit = devices // UNITS
    heads = [flip(my_head, jnp.int32(at), groups) for at in range(groups)]
    shard_ids = [flip(my_pts, jnp.int32(at), shards) for at in range(shards)]

    def peer(slot):
        return heads[slot % groups], shard_ids[mirror(slot // groups, shards)]

    def flat(slot):
        head, pts = peer(slot)
        return head * shards + pts

    def each_peer(step):
        for slot in range(1, devices):
            step(slot)

    def loop(low, high, step):
        def run(at, carry):
            step(at)
            return carry
        lax.fori_loop(low, high, run, 0)

    barrier = pltpu.get_barrier_semaphore()
    load = pltpu.make_async_copy(x_hbm, x_v, local_sem.at[0])
    load.start()
    each_peer(lambda slot: pl.semaphore_signal(
        barrier, 1, device_id=peer(slot), device_id_type=MESH
    ))
    entry_load = pltpu.make_async_copy(entry_hbm, entry_ref, local_sem.at[1])
    exit_load = pltpu.make_async_copy(exit_hbm, exit_ref, local_sem.at[2])
    entry_load.start()
    exit_load.start()

    sharp_v[...] = jnp.zeros_like(sharp_v)
    sharp_v[:, :own] = sharp_ref[...]
    sharp_in[my_head] = sharp_v[...]

    w_ref[:width] = attribute_ref[...].astype(F32).T.astype(BF16)
    w_ref[width:] = feeder_ref[...].astype(F32).T.astype(BF16)
    repeated = jnp.concatenate([project_ref[...].astype(F32).T] * (columns // slices), axis=0)
    lane = lax.broadcasted_iota(I32, (DH, width), 1) % DH
    pick = (lane == lax.broadcasted_iota(I32, (DH, width), 0)).astype(F32).astype(BF16)
    filled = jnp.dot(repeated.astype(BF16), pick, preferred_element_type=F32)
    expand_ref[...] = jnp.where(same_head(filled.shape, slices, DH), filled, 0.0).astype(BF16)
    row = lax.broadcasted_iota(I32, (columns, slices), 0) % slices
    match = row == lax.broadcasted_iota(I32, (columns, slices), 1)
    offset_ref[...] = jnp.sum(jnp.where(match, offset_row_ref[...], 0.0), axis=1, keepdims=True)
    numer[...] = jnp.zeros_like(numer)
    total[...] = jnp.zeros_like(total)

    load.wait()

    def widen(at):
        part = x_v[pl.ds(pl.multiple_of(at * tile, tile), tile), :].astype(F32)
        xf[pl.ds(at * 2 * tile, tile, stride=2), :] = part[:, :LANES]
        xf[pl.ds(at * 2 * tile + 1, tile, stride=2), :] = part[:, LANES:]

    def collect(at):
        for k in range(tile):
            stage[2 * k : 2 * k + 2, :] = xf[
                pl.ds(order_s[at * blocks + k // per_pair, k % per_pair] * 2, 2), :
            ]
        span = pl.ds(pl.multiple_of(at * tile, tile), tile)
        send_v[span, :LANES] = stage[pl.ds(0, tile, stride=2), :].astype(BF16)
        send_v[span, LANES:] = stage[pl.ds(1, tile, stride=2), :].astype(BF16)

    loop(0, STEPS, widen)
    loop(0, STEPS // 2, collect)
    pl.semaphore_wait(barrier, devices - 1)

    def sharp_copy(step):
        return pltpu.make_async_remote_copy(
            sharp_v, sharp_in.at[my_head], sharp_send.at[step], sharp_recv.at[step],
            device_id=(heads[step], my_pts), device_id_type=MESH,
        )

    def meta_copy(slot):
        return pltpu.make_async_remote_copy(
            meta_v.at[slot], meta_in.at[slot], meta_send.at[slot], meta_recv.at[slot],
            device_id=peer(slot), device_id_type=MESH,
        )

    def row_copy(slot, goal):
        span = pl.ds(pl.multiple_of(slot * per_pair, per_pair), per_pair)
        return pltpu.make_async_remote_copy(
            send_v.at[span], recv_v.at[span], row_send.at[slot], row_recv.at[slot],
            device_id=goal, device_id_type=MESH,
        )

    def far_goal(slot):
        shard = mirror(lax.div(slot, groups), shards)
        return flip(my_head, lax.rem(slot, groups), groups), flip(my_pts, shard, shards)

    def send_units(low, high):
        for slot in range(max(low * unit, 1), high * unit):
            row_copy(slot, peer(slot)).start()

    def part_copy(slot):
        return pltpu.make_async_remote_copy(
            part_out.at[flat(slot)], part_in.at[slot], part_send.at[slot], part_recv.at[slot],
            device_id=peer(slot), device_id_type=MESH,
        )

    def all_copy(slot):
        return pltpu.make_async_remote_copy(
            mine, all_in.at[me], all_send.at[slot], all_recv.at[slot],
            device_id=peer(slot), device_id_type=MESH,
        )

    for step in range(1, groups):
        sharp_copy(step).start()
    send_units(0, FIRST)
    loop(STEPS // 2, STEPS, collect)
    for step in range(1, groups):
        sharp_copy(step).wait()
    per_group = own * slices
    for group in range(groups):
        lane = lax.broadcasted_iota(I32, (per_group, LANES), 1)
        member = lax.broadcasted_iota(I32, (per_group, LANES), 0) // slices
        sharp = jnp.sum(jnp.where(lane == member, sharp_in[group], 0.0), axis=1, keepdims=True)
        scale_ref[group * per_group : (group + 1) * per_group] = LOG2E / sharp

    def sums_step(at):
        @pl.when(lax.rem(at * (EARLY - FIRST), STEPS) < EARLY - FIRST)
        def _():
            at_unit = FIRST + lax.div(at * (EARLY - FIRST), STEPS)
            for way in range(unit):
                slot = at_unit * unit + way
                row_copy(slot, far_goal(slot)).start()

        span = pl.ds(pl.multiple_of(at * tile, tile), tile)
        normed = norm_rows(x_v[span, :].astype(F32), gain_ref[...], bias_ref[...])
        both = lax.dot_general(w_ref[...], normed, NT, preferred_element_type=F32).astype(BF16)
        share = slice_weights(
            both[width:], expand_ref[...], offset_ref[...], scale_ref[...], slices
        )
        numer[...] += lax.dot_general(
            both[:width], share.astype(BF16), NT, preferred_element_type=F32
        )
        part = share[:, :LANES]
        for low in range(LANES, tile, LANES):
            part += share[:, low : low + LANES]
        total[...] += part

    loop(0, STEPS, sums_step)

    kept = jnp.where(same_head(numer.shape, DH, slices), numer[...], 0.0)
    sums_v[:DH] = jnp.sum(kept.reshape(-1, DH, columns), axis=0)
    sums_v[DH:] = lax.dot_general(
        jnp.ones((8, LANES), F32), total[...], NT, precision=HIGHEST, preferred_element_type=F32
    )
    per_row = columns // LANES
    depth = part_out.shape[1]
    places = [
        (at // per_row, at % per_row * LANES, at // depth, at % depth)
        for at in range((DH + 1) * per_row)
    ]
    part_out[...] = jnp.zeros_like(part_out)
    for line, low, piece, inner in places:
        part_out[piece, inner : inner + 1, :] = sums_v[line : line + 1, low : low + LANES]
    each_peer(lambda slot: part_copy(slot).start())
    part_in[0] = part_out[me]
    send_units(EARLY, EARLY + MID)
    each_peer(lambda slot: meta_copy(slot).start())
    meta_in[0] = meta_v[0]
    recv_v[:per_pair] = send_v[:per_pair]

    def wait_rows(at):
        for way in range(blocks):
            slot = at * blocks + way

            @pl.when(slot > 0)
            def _():
                row_copy(slot, (my_head, my_pts)).wait_recv()

    def weigh(at):
        x = recv_v[pl.ds(pl.multiple_of(at * tile, tile), tile), :].astype(F32)
        normed = norm_rows(x, gain_ref[...], bias_ref[...])
        feeder = lax.dot_general(
            w_ref[width:], normed, NT, preferred_element_type=F32
        ).astype(BF16)
        share = slice_weights(feeder, expand_ref[...], offset_ref[...], scale_ref[...], slices)
        return share.astype(BF16)

    def weigh_ahead(at):
        wait_rows(at)
        share_v[at] = weigh(at)

    loop(0, AHEAD[0], weigh_ahead)

    each_peer(lambda slot: part_copy(slot).wait())
    mine[...] = jnp.sum(part_in[...], axis=0)
    each_peer(lambda slot: all_copy(slot).start())
    send_units(EARLY + MID, UNITS)
    all_in[me] = mine[...]
    loop(AHEAD[0], AHEAD[1], weigh_ahead)
    each_peer(lambda slot: all_copy(slot).wait())
    for line, low, piece, inner in places:
        sums_v[line : line + 1, low : low + LANES] = all_in[piece, inner : inner + 1, :]

    stok = sums_v[:DH] / (sums_v[DH : DH + 1] + 1e-05)
    query, key, value = (
        jnp.dot(m[...].T, stok, precision=HIGHEST, preferred_element_type=F32)
        for m in (question_ref, lookup_ref, content_ref)
    )
    scores = jnp.dot(key.T, query, precision=HIGHEST, preferred_element_type=F32)
    scores = scores * (1.0 / math.sqrt(DH))
    mask = same_head(scores.shape, slices, slices)
    scores = jnp.where(mask, scores, -jnp.inf)
    powers = jnp.exp(scores - jnp.max(scores, axis=0, keepdims=True))
    attention = powers / jnp.sum(powers, axis=0, keepdims=True)
    sout = jnp.dot(value, attention, precision=HIGHEST, preferred_element_type=F32)
    spread = jnp.concatenate([sout] * (width // DH), axis=0)
    blend[...] = jnp.where(same_head(blend.shape, DH, slices), spread, 0.0).astype(BF16)
    entry_load.wait()
    exit_load.wait()

    def finish(at, share):
        x = recv_v[pl.ds(pl.multiple_of(at * tile, tile), tile), :].astype(F32)
        mixed = jnp.dot(blend[...], share, preferred_element_type=F32)
        y = (
            x
            + jnp.dot(mixed.T.astype(BF16), emit_ref[...], preferred_element_type=F32)
            + emit_bias_ref[...]
        )
        z = norm_rows(y, gain2_ref[...], bias2_ref[...])
        result = y + exit_bias_ref[...]
        for low in range(0, entry_ref.shape[1], width):
            h = jnp.dot(z, entry_ref[:, low : low + width], preferred_element_type=F32)
            g = exact_gelu(h + entry_bias_ref[:, low : low + width]).astype(BF16)
            result += jnp.dot(g, exit_ref[low : low + width], preferred_element_type=F32)
        res[pl.ds(at * 2 * tile, tile, stride=2), :] = result[:, :LANES]
        res[pl.ds(at * 2 * tile + 1, tile, stride=2), :] = result[:, LANES:]
        out_copy(at).start()

    def out_copy(at):
        span = pl.ds(pl.multiple_of(at * 2 * tile, 2 * tile), 2 * tile)
        return pltpu.make_async_copy(res.at[span], res_hbm.at[span], out_sem.at[at])

    loop(0, AHEAD[1], lambda at: finish(at, share_v[at]))

    def rows_step(at):
        wait_rows(at)
        finish(at, weigh(at))

    loop(AHEAD[1], STEPS, rows_step)
    each_peer(lambda slot: meta_copy(slot).wait())
    each_peer(lambda slot: row_copy(slot, peer(slot)).wait_send())
    loop(0, STEPS, lambda at: out_copy(at).wait())


def serve_kernel(spot_s, res_hbm, out_hbm, res, placed, out_v, in_sem, out_sem):
    rows = out_v.shape[0]
    tile = rows // STEPS
    blocks = spot_s.shape[0] // STEPS
    per_pair = tile // blocks

    def res_copy(at):
        span = pl.ds(pl.multiple_of(at * 2 * tile, 2 * tile), 2 * tile)
        return pltpu.make_async_copy(res_hbm.at[span], res.at[span], in_sem.at[at])

    def out_copy(at):
        span = pl.ds(pl.multiple_of(at * tile, tile), tile)
        return pltpu.make_async_copy(out_v.at[span], out_hbm.at[span], out_sem.at[at])

    for at in range(STEPS):
        res_copy(at).start()

    def scatter(at, carry):
        res_copy(at).wait()
        for way in range(blocks):
            slot = at * blocks + way
            for k in range(per_pair):
                spot = pl.multiple_of(spot_s[slot, 0, k] * 2, 2)
                row = pl.multiple_of(at * 2 * tile, 2 * tile) + 2 * (way * per_pair + k)
                placed[pl.ds(spot, 2), :] = res[pl.ds(pl.multiple_of(row, 2), 2), :]
        return carry

    lax.fori_loop(0, STEPS, scatter, 0)

    def narrow(at, carry):
        span = pl.ds(pl.multiple_of(at * tile, tile), tile)
        out_v[span, :LANES] = placed[pl.ds(at * 2 * tile, tile, stride=2), :].astype(BF16)
        out_v[span, LANES:] = placed[pl.ds(at * 2 * tile + 1, tile, stride=2), :].astype(BF16)
        out_copy(at).start()
        return carry

    lax.fori_loop(0, STEPS, narrow, 0)
    for at in range(STEPS):
        out_copy(at).wait()


def body(
    layer_inputs_trainorder,
    inference_placement,
    initial_layernorm_gain,
    initial_layernorm_offset,
    attribute_projection,
    assignment_feeder_projection,
    partition_projection,
    partition_offset,
    softmax_sharpness,
    partition_question_map,
    partition_lookup_map,
    partition_content_map,
    emitted_projection,
    emitted_offset,
    latter_layernorm_gain,
    latter_layernorm_offset,
    perceptron_entry_map,
    perceptron_entry_offset,
    perceptron_exit_map,
    perceptron_exit_offset,
):
    groups = lax.axis_size("head")
    shards = lax.axis_size("pts")
    devices = groups * shards
    rows, width = layer_inputs_trainorder.shape
    per_pair = rows // devices
    slices = partition_projection.shape[1]
    columns = softmax_sharpness.shape[0] * groups * slices
    wide = -(-per_pair // LANES) * LANES
    tile = rows // STEPS
    depth = -(-(DH + 1) * (columns // LANES) // devices)
    order, spots = pl.pallas_call(
        functools.partial(index_kernel, groups, shards, rows),
        out_shape=(
            jax.ShapeDtypeStruct((devices, wide), I32),
            jax.ShapeDtypeStruct((devices, 1, wide), I32),
        ),
        scratch_shapes=[pltpu.VMEM((1, rows), I32)] * 3,
    )(inference_placement[None])
    operands = (
        order, spots, softmax_sharpness[None], initial_layernorm_gain[None],
        initial_layernorm_offset[None], attribute_projection, assignment_feeder_projection,
        partition_projection, partition_offset[None], partition_question_map,
        partition_lookup_map, partition_content_map, emitted_projection, emitted_offset[None],
        latter_layernorm_gain[None], latter_layernorm_offset[None],
        perceptron_entry_offset[None], perceptron_exit_offset[None], perceptron_entry_map,
        perceptron_exit_map,
    )
    dma = pltpu.SemaphoreType.DMA
    scratch = [
        pltpu.VMEM((rows, width), BF16),
        pltpu.VMEM((2 * rows, LANES), F32),
        pltpu.VMEM((2 * tile, LANES), F32),
        pltpu.VMEM((rows, width), BF16),
        pltpu.VMEM((rows, width), BF16),
        pltpu.VMEM((2 * rows, LANES), F32),
        pltpu.VMEM((AHEAD[1], columns, tile), BF16),
        pltpu.VMEM(perceptron_entry_map.shape, BF16),
        pltpu.VMEM(perceptron_exit_map.shape, BF16),
        pltpu.VMEM((1, LANES), F32),
        pltpu.VMEM((groups, 1, LANES), F32),
        pltpu.VMEM((2 * width, width), BF16),
        pltpu.VMEM((columns, width), BF16),
        pltpu.VMEM((columns, 1), F32),
        pltpu.VMEM((columns, 1), F32),
        pltpu.VMEM((width, columns), F32),
        pltpu.VMEM((columns, LANES), F32),
        pltpu.VMEM((devices, depth, LANES), F32),
        pltpu.VMEM((devices, depth, LANES), F32),
        pltpu.VMEM((depth, LANES), F32),
        pltpu.VMEM((devices, depth, LANES), F32),
        pltpu.VMEM((DH + 8, columns), F32),
        pltpu.VMEM((width, columns), BF16),
        dma((3,)),
        dma((STEPS,)),
        dma((devices,)),
        dma((devices,)),
        dma((devices,)),
        dma((devices,)),
        dma((groups,)),
        dma((groups,)),
        dma((devices,)),
        dma((devices,)),
        dma((devices,)),
        dma((devices,)),
    ]
    in_vmem = pl.BlockSpec(memory_space=pltpu.VMEM)
    res, arrived = pl.pallas_call(
        functools.partial(fused_kernel, slices, groups, shards),
        out_shape=(
            jax.ShapeDtypeStruct((2 * rows, LANES), F32),
            jax.ShapeDtypeStruct((devices, 1, wide), I32),
        ),
        in_specs=[pl.BlockSpec(memory_space=pl.ANY), pl.BlockSpec(memory_space=pltpu.SMEM)]
        + [in_vmem] * (len(operands) - 3)
        + [pl.BlockSpec(memory_space=pl.ANY)] * 2,
        out_specs=(pl.BlockSpec(memory_space=pl.ANY), in_vmem),
        scratch_shapes=scratch,
        compiler_params=pltpu.CompilerParams(
            collective_id=0, has_side_effects=True, vmem_limit_bytes=60 * 2**20
        ),
        cost_estimate=pl.CostEstimate(
            flops=rows * width * columns * 24, bytes_accessed=rows * width * 8,
            transcendentals=rows * columns * 4,
        ),
    )(layer_inputs_trainorder, *operands)
    anywhere = pl.BlockSpec(memory_space=pl.ANY)
    out = pl.pallas_call(
        serve_kernel,
        in_specs=[pl.BlockSpec(memory_space=pltpu.SMEM), anywhere],
        out_specs=anywhere,
        out_shape=jax.ShapeDtypeStruct((rows, width), BF16),
        scratch_shapes=[
            pltpu.VMEM((2 * rows, LANES), F32),
            pltpu.VMEM((2 * rows, LANES), F32),
            pltpu.VMEM((rows, width), BF16),
            dma((STEPS,)),
            dma((STEPS,)),
        ],
    )(arrived, res)
    return out[None]


def solution(mesh):
    placed = (
        P(("head", "pts"), None),
        P(("head", "pts")),
        P(),
        P(),
        P(),
        P(),
        P(),
        P(),
        P("head"),
        P(),
        P(),
        P(),
        P(),
        P(),
        P(),
        P(),
        P(),
        P(),
        P(),
        P(),
    )
    return jax.shard_map(
        body, mesh=mesh, in_specs=placed, out_specs=P("pts", "head", None), check_vma=False
    )
```

```python
import functools
import math

import jax
import jax.numpy as jnp
from jax import lax
from jax.experimental import pallas as pl
from jax.experimental.pallas import tpu as pltpu
from jax.sharding import PartitionSpec as P

DH = 16
LANES = 128
STEPS = 16
SUM_STEPS = 12
PARTS = 4
UNITS = 32
FIRST = 8
EARLY = 12
MID = 3
AHEAD = (4, 7)
F32 = jnp.float32
BF16 = jnp.bfloat16
I32 = jnp.int32
HIGHEST = lax.Precision.HIGHEST
LOG2E = math.log2(math.e)
NT = (((1,), (1,)), ((), ()))
MESH = pl.DeviceIdType.MESH


def norm_rows(rows, gain, bias):
    mean = jnp.mean(rows, axis=-1, keepdims=True)
    centred = rows - mean
    spread = jnp.mean(centred * centred, axis=-1, keepdims=True)
    return (centred * lax.rsqrt(spread + 1e-05) * gain + bias).astype(BF16)


def slice_weights(feeder_t, expand, offset, scale, slices):
    raw = jnp.dot(expand, feeder_t, preferred_element_type=F32)
    logit = (raw + offset) * scale
    lanes = logit.shape[1]
    logit = logit.reshape(-1, slices, lanes)
    powers = jnp.exp2(logit - jnp.max(logit, axis=1, keepdims=True))
    share = powers * (1.0 / jnp.sum(powers, axis=1, keepdims=True))
    return share.reshape(-1, lanes)


def same_head(shape, row_size, column_size):
    row_head = lax.broadcasted_iota(I32, shape, 0) // row_size
    column_head = lax.broadcasted_iota(I32, shape, 1) // column_size
    return row_head == column_head


def exact_gelu(h):
    half = 0.5 * h
    return half + half * lax.erf(h * (1.0 / math.sqrt(2.0)))


def floor_div(value, divisor):
    return ((value.astype(F32) + 0.5) * (1.0 / divisor)).astype(I32)


def flip(a, b, size):
    result, bit = 0, 1
    while bit < size:
        result = result + lax.rem(lax.div(a, bit) + lax.div(b, bit), 2) * bit
        bit *= 2
    return result


def mirror(a, size):
    result, low, high = 0, 1, size // 2
    while high >= 1:
        if isinstance(a, int):
            result = result + a // low % 2 * high
        else:
            result = result + lax.rem(lax.div(a, low), 2) * high
        low, high = low * 2, high // 2
    return result


def index_kernel(groups, shards, rows, place_ref, order_ref, spots_ref, rank_v, target_v, spot_v):
    devices = groups * shards
    chunks = rows // LANES

    place = place_ref[...]
    block = floor_div(place, rows)
    shard = floor_div(block, groups)
    apart = (block - shard * groups) ^ lax.axis_index("head")
    shard = shard ^ lax.axis_index("pts")
    bits = shards.bit_length() - 1
    shard = sum(((shard >> at) & 1) << (bits - 1 - at) for at in range(bits))
    target = shard * groups + apart
    target_v[...] = target
    spot_v[...] = place - block * rows
    upper = (
        lax.broadcasted_iota(I32, (LANES, LANES), 0) <= lax.broadcasted_iota(I32, (LANES, LANES), 1)
    ).astype(F32).astype(BF16)
    stacked = jnp.concatenate(
        [
            (lax.broadcasted_iota(I32, (devices, LANES), 0)
             == target[:, at * LANES : (at + 1) * LANES]).astype(F32)
            for at in range(chunks)
        ],
        axis=0,
    )
    prefix = jnp.dot(stacked.astype(BF16), upper, preferred_element_type=F32)
    run = jnp.zeros((devices, 1), F32)
    for at in range(chunks):
        span = slice(at * devices, (at + 1) * devices)
        ahead = jnp.sum(stacked[span] * (prefix[span] + (run - 1.0)), axis=0, keepdims=True)
        rank_v[:, at * LANES : (at + 1) * LANES] = ahead.astype(I32)
        run = run + prefix[span][:, LANES - 1 :]

    per_pair = order_ref.shape[1]
    part_lanes = 8 * LANES

    def invert(at, total_so_far):
        lanes = pl.ds(pl.multiple_of(at * part_lanes, part_lanes), part_lanes)
        hot = (
            lax.broadcasted_iota(I32, (devices, part_lanes), 0) == target_v[:, lanes]
        ).astype(F32)
        slot_hot = (
            lax.broadcasted_iota(I32, (per_pair, part_lanes), 0) == rank_v[:, lanes]
        ).astype(F32).astype(BF16)
        index = lax.broadcasted_iota(I32, (1, part_lanes), 1) + at * part_lanes
        values = []
        for value in (index, spot_v[:, lanes]):
            high = value // 64
            values += [hot * high.astype(F32), hot * (value - high * 64).astype(F32)]
        values = jnp.concatenate(values, axis=0).astype(BF16)
        return total_so_far + lax.dot_general(values, slot_hot, NT, preferred_element_type=F32)

    table = lax.fori_loop(
        0, rows // part_lanes, invert, jnp.zeros((4 * devices, per_pair), F32)
    )
    order_ref[...] = (table[:devices] * 128.0 + table[devices : 2 * devices] * 2.0).astype(I32)
    spots = table[2 * devices : 3 * devices] * 128.0 + table[3 * devices :] * 2.0
    spots_ref[...] = jnp.zeros_like(spots_ref)
    for at in range(devices):
        spots_ref[at, :, :per_pair] = spots[at : at + 1].astype(I32)


def fused_kernel(
    slices, groups, shards,
    x_hbm, order_s, meta_v, sharp_ref, gain_ref, bias_ref, attribute_ref, feeder_ref, project_ref,
    offset_row_ref, question_ref, lookup_ref, content_ref, emit_ref, emit_bias_ref,
    gain2_ref, bias2_ref, entry_bias_ref, exit_bias_ref, entry_hbm, exit_hbm,
    res_hbm, meta_in,
    x_v, xf, stage, send_v, recv_v, res, share_v, entry_ref, exit_ref,
    sharp_v, sharp_in, w_ref, expand_ref, offset_ref, scale_ref, numer, total,
    part_out, part_in, mine, all_in, sums_v, blend,
    local_sem, out_sem, row_send, row_recv, meta_send, meta_recv, sharp_send, sharp_recv,
    part_send, part_recv, all_send, all_recv,
):
    devices = groups * shards
    rows, width = x_v.shape
    per_pair = rows // devices
    tile = rows // STEPS
    blocks = devices // STEPS
    sum_tile = rows // SUM_STEPS
    columns = expand_ref.shape[0]
    own = sharp_ref.shape[1]
    my_head, my_pts = lax.axis_index("head"), lax.axis_index("pts")
    me = my_head * shards + my_pts

    unit = devices // UNITS
    heads = [flip(my_head, jnp.int32(at), groups) for at in range(groups)]
    shard_ids = [flip(my_pts, jnp.int32(at), shards) for at in range(shards)]

    def peer(slot):
        return heads[slot % groups], shard_ids[mirror(slot // groups, shards)]

    def flat(slot):
        head, pts = peer(slot)
        return head * shards + pts

    def each_peer(step):
        for slot in range(1, devices):
            step(slot)

    def loop(low, high, step):
        def run(at, carry):
            step(at)
            return carry
        lax.fori_loop(low, high, run, 0)

    barrier = pltpu.get_barrier_semaphore()
    load = pltpu.make_async_copy(x_hbm, x_v, local_sem.at[0])
    load.start()
    each_peer(lambda slot: pl.semaphore_signal(
        barrier, 1, device_id=peer(slot), device_id_type=MESH
    ))
    entry_load = pltpu.make_async_copy(entry_hbm, entry_ref, local_sem.at[1])
    exit_load = pltpu.make_async_copy(exit_hbm, exit_ref, local_sem.at[2])
    entry_load.start()
    exit_load.start()

    sharp_v[...] = jnp.zeros_like(sharp_v)
    sharp_v[:, :own] = sharp_ref[...]
    sharp_in[my_head] = sharp_v[...]

    w_ref[:width] = attribute_ref[...].astype(F32).T.astype(BF16)
    w_ref[width:] = feeder_ref[...].astype(F32).T.astype(BF16)
    repeated = jnp.concatenate([project_ref[...].astype(F32).T] * (columns // slices), axis=0)
    lane = lax.broadcasted_iota(I32, (DH, width), 1) % DH
    pick = (lane == lax.broadcasted_iota(I32, (DH, width), 0)).astype(F32).astype(BF16)
    filled = jnp.dot(repeated.astype(BF16), pick, preferred_element_type=F32)
    expand_ref[...] = jnp.where(same_head(filled.shape, slices, DH), filled, 0.0).astype(BF16)
    row = lax.broadcasted_iota(I32, (columns, slices), 0) % slices
    match = row == lax.broadcasted_iota(I32, (columns, slices), 1)
    offset_ref[...] = jnp.sum(jnp.where(match, offset_row_ref[...], 0.0), axis=1, keepdims=True)
    numer[...] = jnp.zeros_like(numer)
    total[...] = jnp.zeros_like(total)

    load.wait()

    def widen(at):
        part = x_v[pl.ds(pl.multiple_of(at * tile, tile), tile), :].astype(F32)
        xf[pl.ds(at * 2 * tile, tile, stride=2), :] = part[:, :LANES]
        xf[pl.ds(at * 2 * tile + 1, tile, stride=2), :] = part[:, LANES:]

    def collect(at):
        for way in range(blocks):
            def take(k, carry):
                put = pl.multiple_of(2 * (way * per_pair + k), 2)
                stage[pl.ds(put, 2), :] = xf[pl.ds(order_s[at * blocks + way, k], 2), :]
                return carry
            lax.fori_loop(0, per_pair, take, 0, unroll=True)
        span = slice(at * tile, (at + 1) * tile)
        send_v[span, :LANES] = stage[pl.ds(0, tile, stride=2), :].astype(BF16)
        send_v[span, LANES:] = stage[pl.ds(1, tile, stride=2), :].astype(BF16)

    loop(0, STEPS, widen)
    for at in range(STEPS // 2):
        collect(at)
    pl.semaphore_wait(barrier, devices - 1)

    def sharp_copy(step):
        return pltpu.make_async_remote_copy(
            sharp_v, sharp_in.at[my_head], sharp_send.at[step], sharp_recv.at[step],
            device_id=(heads[step], my_pts), device_id_type=MESH,
        )

    def meta_copy(slot):
        return pltpu.make_async_remote_copy(
            meta_v.at[slot], meta_in.at[slot], meta_send.at[slot], meta_recv.at[slot],
            device_id=peer(slot), device_id_type=MESH,
        )

    def row_copy(slot, goal):
        span = pl.ds(pl.multiple_of(slot * per_pair, per_pair), per_pair)
        return pltpu.make_async_remote_copy(
            send_v.at[span], recv_v.at[span], row_send.at[slot], row_recv.at[slot],
            device_id=goal, device_id_type=MESH,
        )

    def far_goal(slot):
        shard = mirror(lax.div(slot, groups), shards)
        return flip(my_head, lax.rem(slot, groups), groups), flip(my_pts, shard, shards)

    def send_units(low, high):
        for slot in range(max(low * unit, 1), high * unit):
            row_copy(slot, peer(slot)).start()

    def part_copy(slot):
        return pltpu.make_async_remote_copy(
            part_out.at[flat(slot)], part_in.at[slot], part_send.at[slot], part_recv.at[slot],
            device_id=peer(slot), device_id_type=MESH,
        )

    def all_copy(slot):
        return pltpu.make_async_remote_copy(
            mine, all_in.at[me], all_send.at[slot], all_recv.at[slot],
            device_id=peer(slot), device_id_type=MESH,
        )

    for step in range(1, groups):
        sharp_copy(step).start()
    send_units(0, FIRST)
    for at in range(STEPS // 2, STEPS):
        collect(at)
    for step in range(1, groups):
        sharp_copy(step).wait()
    per_group = own * slices
    for group in range(groups):
        lane = lax.broadcasted_iota(I32, (per_group, LANES), 1)
        member = lax.broadcasted_iota(I32, (per_group, LANES), 0) // slices
        sharp = jnp.sum(jnp.where(lane == member, sharp_in[group], 0.0), axis=1, keepdims=True)
        scale_ref[group * per_group : (group + 1) * per_group] = LOG2E / sharp

    def sums_step(at):
        @pl.when(lax.rem(at * (EARLY - FIRST), SUM_STEPS) < EARLY - FIRST)
        def _():
            at_unit = FIRST + lax.div(at * (EARLY - FIRST), SUM_STEPS)
            for way in range(unit):
                slot = at_unit * unit + way
                row_copy(slot, far_goal(slot)).start()

        span = pl.ds(pl.multiple_of(at * sum_tile, sum_tile), sum_tile)
        normed = norm_rows(x_v[span, :].astype(F32), gain_ref[...], bias_ref[...])
        both = lax.dot_general(w_ref[...], normed, NT, preferred_element_type=F32).astype(BF16)
        share = slice_weights(
            both[width:], expand_ref[...], offset_ref[...], scale_ref[...], slices
        )
        numer[...] += lax.dot_general(
            both[:width], share.astype(BF16), NT, preferred_element_type=F32
        )
        part = share[:, :LANES]
        for low in range(LANES, sum_tile, LANES):
            part += share[:, low : low + LANES]
        total[...] += part

    loop(0, SUM_STEPS, sums_step)

    kept = jnp.where(same_head(numer.shape, DH, slices), numer[...], 0.0)
    sums_v[:DH] = jnp.sum(kept.reshape(-1, DH, columns), axis=0)
    sums_v[DH:] = lax.dot_general(
        jnp.ones((8, LANES), F32), total[...], NT, precision=HIGHEST, preferred_element_type=F32
    )
    per_row = columns // LANES
    depth = part_out.shape[1]
    places = [
        (at // per_row, at % per_row * LANES, at // depth, at % depth)
        for at in range((DH + 1) * per_row)
    ]
    part_out[...] = jnp.zeros_like(part_out)
    for line, low, piece, inner in places:
        part_out[piece, inner : inner + 1, :] = sums_v[line : line + 1, low : low + LANES]
    each_peer(lambda slot: part_copy(slot).start())
    part_in[0] = part_out[me]
    send_units(EARLY, EARLY + MID)
    each_peer(lambda slot: meta_copy(slot).start())
    meta_in[0] = meta_v[0]
    recv_v[:per_pair] = send_v[:per_pair]

    def wait_rows(at):
        for way in range(blocks):
            slot = at * blocks + way

            @pl.when(slot > 0)
            def _():
                row_copy(slot, (my_head, my_pts)).wait_recv()

    def weigh(at):
        x = recv_v[pl.ds(pl.multiple_of(at * tile, tile), tile), :].astype(F32)
        normed = norm_rows(x, gain_ref[...], bias_ref[...])
        feeder = lax.dot_general(
            w_ref[width:], normed, NT, preferred_element_type=F32
        ).astype(BF16)
        share = slice_weights(feeder, expand_ref[...], offset_ref[...], scale_ref[...], slices)
        return share.astype(BF16)

    def weigh_ahead(at):
        wait_rows(at)
        share_v[at] = weigh(at)

    loop(0, AHEAD[0], weigh_ahead)

    each_peer(lambda slot: part_copy(slot).wait())
    mine[...] = jnp.sum(part_in[...], axis=0)
    each_peer(lambda slot: all_copy(slot).start())
    send_units(EARLY + MID, UNITS)
    all_in[me] = mine[...]
    loop(AHEAD[0], AHEAD[1], weigh_ahead)
    each_peer(lambda slot: all_copy(slot).wait())
    for line, low, piece, inner in places:
        sums_v[line : line + 1, low : low + LANES] = all_in[piece, inner : inner + 1, :]

    stok = sums_v[:DH] / (sums_v[DH : DH + 1] + 1e-05)
    query, key, value = (
        jnp.dot(m[...].T, stok, precision=HIGHEST, preferred_element_type=F32)
        for m in (question_ref, lookup_ref, content_ref)
    )
    scores = jnp.dot(key.T, query, precision=HIGHEST, preferred_element_type=F32)
    scores = scores * (1.0 / math.sqrt(DH))
    mask = same_head(scores.shape, slices, slices)
    scores = jnp.where(mask, scores, -jnp.inf)
    powers = jnp.exp(scores - jnp.max(scores, axis=0, keepdims=True))
    attention = powers / jnp.sum(powers, axis=0, keepdims=True)
    sout = jnp.dot(value, attention, precision=HIGHEST, preferred_element_type=F32)
    spread = jnp.concatenate([sout] * (width // DH), axis=0)
    blend[...] = jnp.where(same_head(blend.shape, DH, slices), spread, 0.0).astype(BF16)
    entry_load.wait()
    exit_load.wait()

    def finish(at, share):
        x = recv_v[pl.ds(pl.multiple_of(at * tile, tile), tile), :].astype(F32)
        mixed = jnp.dot(blend[...], share, preferred_element_type=F32)
        y = (
            x
            + jnp.dot(mixed.T.astype(BF16), emit_ref[...], preferred_element_type=F32)
            + emit_bias_ref[...]
        )
        z = norm_rows(y, gain2_ref[...], bias2_ref[...])
        result = y + exit_bias_ref[...]
        for low in range(0, entry_ref.shape[1], width):
            h = jnp.dot(z, entry_ref[:, low : low + width], preferred_element_type=F32)
            g = exact_gelu(h + entry_bias_ref[:, low : low + width]).astype(BF16)
            result += jnp.dot(g, exit_ref[low : low + width], preferred_element_type=F32)
        res[pl.ds(at * 2 * tile, tile, stride=2), :] = result[:, :LANES]
        res[pl.ds(at * 2 * tile + 1, tile, stride=2), :] = result[:, LANES:]
        out_copy(at).start()

    def out_copy(at):
        span = pl.ds(pl.multiple_of(at * 2 * tile, 2 * tile), 2 * tile)
        return pltpu.make_async_copy(res.at[span], res_hbm.at[span], out_sem.at[at])

    loop(0, AHEAD[1], lambda at: finish(at, share_v[at]))

    def rows_step(at):
        wait_rows(at)
        finish(at, weigh(at))

    loop(AHEAD[1], STEPS, rows_step)
    each_peer(lambda slot: meta_copy(slot).wait())
    each_peer(lambda slot: row_copy(slot, peer(slot)).wait_send())
    loop(0, STEPS, lambda at: out_copy(at).wait())


def serve_kernel(spot_s, res_hbm, out_hbm, res, placed, out_v, in_sem, out_sem):
    rows = out_v.shape[0]
    tile = rows // STEPS
    part = rows // PARTS
    blocks = spot_s.shape[0] // STEPS
    per_pair = tile // blocks

    def res_copy(at):
        span = pl.ds(pl.multiple_of(at * 2 * tile, 2 * tile), 2 * tile)
        return pltpu.make_async_copy(res_hbm.at[span], res.at[span], in_sem.at[at])

    def out_copy(at):
        span = pl.ds(pl.multiple_of(at * part, part), part)
        return pltpu.make_async_copy(out_v.at[span], out_hbm.at[span], out_sem.at[at])

    for at in range(STEPS):
        res_copy(at).start()

    for at in range(STEPS):
        res_copy(at).wait()
        for slot in range(at * blocks, (at + 1) * blocks):
            def put(k, carry):
                spot = pl.multiple_of(spot_s[slot, 0, k], 2)
                low = pl.multiple_of(2 * (slot * per_pair + k), 2)
                placed[pl.ds(spot, 2), :] = res[pl.ds(low, 2), :]
                return carry
            lax.fori_loop(0, per_pair, put, 0, unroll=True)

    def narrow(at, carry):
        first = at * 2 * part
        span = pl.ds(pl.multiple_of(at * part, part), part)
        out_v[span, :LANES] = placed[pl.ds(first, part, stride=2), :].astype(BF16)
        out_v[span, LANES:] = placed[pl.ds(first + 1, part, stride=2), :].astype(BF16)
        out_copy(at).start()
        return carry

    lax.fori_loop(0, PARTS, narrow, 0)
    for at in range(PARTS):
        out_copy(at).wait()


def body(
    layer_inputs_trainorder,
    inference_placement,
    initial_layernorm_gain,
    initial_layernorm_offset,
    attribute_projection,
    assignment_feeder_projection,
    partition_projection,
    partition_offset,
    softmax_sharpness,
    partition_question_map,
    partition_lookup_map,
    partition_content_map,
    emitted_projection,
    emitted_offset,
    latter_layernorm_gain,
    latter_layernorm_offset,
    perceptron_entry_map,
    perceptron_entry_offset,
    perceptron_exit_map,
    perceptron_exit_offset,
):
    groups = lax.axis_size("head")
    shards = lax.axis_size("pts")
    devices = groups * shards
    rows, width = layer_inputs_trainorder.shape
    per_pair = rows // devices
    slices = partition_projection.shape[1]
    columns = softmax_sharpness.shape[0] * groups * slices
    wide = -(-per_pair // LANES) * LANES
    tile = rows // STEPS
    depth = -(-(DH + 1) * (columns // LANES) // devices)
    order, spots = pl.pallas_call(
        functools.partial(index_kernel, groups, shards, rows),
        out_shape=(
            jax.ShapeDtypeStruct((devices, per_pair), I32),
            jax.ShapeDtypeStruct((devices, 1, wide), I32),
        ),
        scratch_shapes=[pltpu.VMEM((1, rows), I32)] * 3,
    )(inference_placement[None])
    operands = (
        order, spots, softmax_sharpness[None], initial_layernorm_gain[None],
        initial_layernorm_offset[None], attribute_projection, assignment_feeder_projection,
        partition_projection, partition_offset[None], partition_question_map,
        partition_lookup_map, partition_content_map, emitted_projection, emitted_offset[None],
        latter_layernorm_gain[None], latter_layernorm_offset[None],
        perceptron_entry_offset[None], perceptron_exit_offset[None], perceptron_entry_map,
        perceptron_exit_map,
    )
    dma = pltpu.SemaphoreType.DMA
    scratch = [
        pltpu.VMEM((rows, width), BF16),
        pltpu.VMEM((2 * rows, LANES), F32),
        pltpu.VMEM((2 * tile, LANES), F32),
        pltpu.VMEM((rows, width), BF16),
        pltpu.VMEM((rows, width), BF16),
        pltpu.VMEM((2 * rows, LANES), F32),
        pltpu.VMEM((AHEAD[1], columns, tile), BF16),
        pltpu.VMEM(perceptron_entry_map.shape, BF16),
        pltpu.VMEM(perceptron_exit_map.shape, BF16),
        pltpu.VMEM((1, LANES), F32),
        pltpu.VMEM((groups, 1, LANES), F32),
        pltpu.VMEM((2 * width, width), BF16),
        pltpu.VMEM((columns, width), BF16),
        pltpu.VMEM((columns, 1), F32),
        pltpu.VMEM((columns, 1), F32),
        pltpu.VMEM((width, columns), F32),
        pltpu.VMEM((columns, LANES), F32),
        pltpu.VMEM((devices, depth, LANES), F32),
        pltpu.VMEM((devices, depth, LANES), F32),
        pltpu.VMEM((depth, LANES), F32),
        pltpu.VMEM((devices, depth, LANES), F32),
        pltpu.VMEM((DH + 8, columns), F32),
        pltpu.VMEM((width, columns), BF16),
        dma((3,)),
        dma((STEPS,)),
        dma((devices,)),
        dma((devices,)),
        dma((devices,)),
        dma((devices,)),
        dma((groups,)),
        dma((groups,)),
        dma((devices,)),
        dma((devices,)),
        dma((devices,)),
        dma((devices,)),
    ]
    in_vmem = pl.BlockSpec(memory_space=pltpu.VMEM)
    res, arrived = pl.pallas_call(
        functools.partial(fused_kernel, slices, groups, shards),
        out_shape=(
            jax.ShapeDtypeStruct((2 * rows, LANES), F32),
            jax.ShapeDtypeStruct((devices, 1, wide), I32),
        ),
        in_specs=[pl.BlockSpec(memory_space=pl.ANY), pl.BlockSpec(memory_space=pltpu.SMEM)]
        + [in_vmem] * (len(operands) - 3)
        + [pl.BlockSpec(memory_space=pl.ANY)] * 2,
        out_specs=(pl.BlockSpec(memory_space=pl.ANY), in_vmem),
        scratch_shapes=scratch,
        compiler_params=pltpu.CompilerParams(
            collective_id=0, has_side_effects=True, vmem_limit_bytes=60 * 2**20
        ),
        cost_estimate=pl.CostEstimate(
            flops=rows * width * columns * 24, bytes_accessed=rows * width * 8,
            transcendentals=rows * columns * 4,
        ),
    )(layer_inputs_trainorder, *operands)
    anywhere = pl.BlockSpec(memory_space=pl.ANY)
    out = pl.pallas_call(
        serve_kernel,
        in_specs=[pl.BlockSpec(memory_space=pltpu.SMEM), anywhere],
        out_specs=anywhere,
        out_shape=jax.ShapeDtypeStruct((rows, width), BF16),
        scratch_shapes=[
            pltpu.VMEM((2 * rows, LANES), F32),
            pltpu.VMEM((2 * rows, LANES), F32),
            pltpu.VMEM((rows, width), BF16),
            dma((STEPS,)),
            dma((PARTS,)),
        ],
    )(arrived, res)
    return out[None]


def solution(mesh):
    placed = (
        P(("head", "pts"), None),
        P(("head", "pts")),
        P(),
        P(),
        P(),
        P(),
        P(),
        P(),
        P("head"),
        P(),
        P(),
        P(),
        P(),
        P(),
        P(),
        P(),
        P(),
        P(),
        P(),
        P(),
    )
    return jax.shard_map(
        body, mesh=mesh, in_specs=placed, out_specs=P("pts", "head", None), check_vma=False
    )
```

```python
import functools
import math

import jax
import jax.numpy as jnp
from jax import lax
from jax.experimental import pallas as pl
from jax.experimental.pallas import tpu as pltpu
from jax.sharding import PartitionSpec as P

DH = 16
LANES = 128
STEPS = 16
SUM_STEPS = 12
PARTS = 4
UNITS = 32
FIRST = 8
EARLY = 11
MID = 1
AHEAD = (3, 8)
F32 = jnp.float32
BF16 = jnp.bfloat16
I32 = jnp.int32
HIGHEST = lax.Precision.HIGHEST
LOG2E = math.log2(math.e)
NT = (((1,), (1,)), ((), ()))
MESH = pl.DeviceIdType.MESH


def norm_rows(rows, gain, bias):
    mean = jnp.mean(rows, axis=-1, keepdims=True)
    centred = rows - mean
    spread = jnp.mean(centred * centred, axis=-1, keepdims=True)
    return (centred * lax.rsqrt(spread + 1e-05) * gain + bias).astype(BF16)


def slice_weights(feeder_t, expand, offset, scale, slices):
    raw = jnp.dot(expand, feeder_t, preferred_element_type=F32)
    logit = (raw + offset) * scale
    lanes = logit.shape[1]
    logit = logit.reshape(-1, slices, lanes)
    powers = jnp.exp2(logit - jnp.max(logit, axis=1, keepdims=True))
    share = powers * (1.0 / jnp.sum(powers, axis=1, keepdims=True))
    return share.reshape(-1, lanes)


def same_head(shape, row_size, column_size):
    row_head = lax.broadcasted_iota(I32, shape, 0) // row_size
    column_head = lax.broadcasted_iota(I32, shape, 1) // column_size
    return row_head == column_head


def exact_gelu(h):
    half = 0.5 * h
    return half + half * lax.erf(h * (1.0 / math.sqrt(2.0)))


def floor_div(value, divisor):
    return ((value.astype(F32) + 0.5) * (1.0 / divisor)).astype(I32)


def flip(a, b, size):
    result, bit = 0, 1
    while bit < size:
        result = result + lax.rem(lax.div(a, bit) + lax.div(b, bit), 2) * bit
        bit *= 2
    return result


def mirror(a, size):
    result, low, high = 0, 1, size // 2
    while high >= 1:
        if isinstance(a, int):
            result = result + a // low % 2 * high
        else:
            result = result + lax.rem(lax.div(a, low), 2) * high
        low, high = low * 2, high // 2
    return result


def index_kernel(groups, shards, rows, place_ref, order_ref, spots_ref, rank_v, target_v, spot_v):
    devices = groups * shards
    chunks = rows // LANES

    place = place_ref[...]
    block = floor_div(place, rows)
    shard = floor_div(block, groups)
    apart = (block - shard * groups) ^ lax.axis_index("head")
    shard = shard ^ lax.axis_index("pts")
    bits = shards.bit_length() - 1
    shard = sum(((shard >> at) & 1) << (bits - 1 - at) for at in range(bits))
    target = shard * groups + apart
    target_v[...] = target
    spot_v[...] = place - block * rows
    upper = (
        lax.broadcasted_iota(I32, (LANES, LANES), 0) <= lax.broadcasted_iota(I32, (LANES, LANES), 1)
    ).astype(F32).astype(BF16)
    stacked = jnp.concatenate(
        [
            (lax.broadcasted_iota(I32, (devices, LANES), 0)
             == target[:, at * LANES : (at + 1) * LANES]).astype(F32)
            for at in range(chunks)
        ],
        axis=0,
    )
    prefix = jnp.dot(stacked.astype(BF16), upper, preferred_element_type=F32)
    run = jnp.zeros((devices, 1), F32)
    for at in range(chunks):
        span = slice(at * devices, (at + 1) * devices)
        ahead = jnp.sum(stacked[span] * (prefix[span] + (run - 1.0)), axis=0, keepdims=True)
        rank_v[:, at * LANES : (at + 1) * LANES] = ahead.astype(I32)
        run = run + prefix[span][:, LANES - 1 :]

    per_pair = order_ref.shape[1]
    part_lanes = 8 * LANES

    def invert(at, total_so_far):
        lanes = pl.ds(pl.multiple_of(at * part_lanes, part_lanes), part_lanes)
        hot = (
            lax.broadcasted_iota(I32, (devices, part_lanes), 0) == target_v[:, lanes]
        ).astype(F32)
        slot_hot = (
            lax.broadcasted_iota(I32, (per_pair, part_lanes), 0) == rank_v[:, lanes]
        ).astype(F32).astype(BF16)
        index = lax.broadcasted_iota(I32, (1, part_lanes), 1) + at * part_lanes
        values = []
        for value in (index, spot_v[:, lanes]):
            high = value // 64
            values += [hot * high.astype(F32), hot * (value - high * 64).astype(F32)]
        values = jnp.concatenate(values, axis=0).astype(BF16)
        return total_so_far + lax.dot_general(values, slot_hot, NT, preferred_element_type=F32)

    table = lax.fori_loop(
        0, rows // part_lanes, invert, jnp.zeros((4 * devices, per_pair), F32)
    )
    order_ref[...] = (table[:devices] * 128.0 + table[devices : 2 * devices] * 2.0).astype(I32)
    spots = table[2 * devices : 3 * devices] * 128.0 + table[3 * devices :] * 2.0
    spots_ref[...] = jnp.zeros_like(spots_ref)
    for at in range(devices):
        spots_ref[at, :, :per_pair] = spots[at : at + 1].astype(I32)


def fused_kernel(
    slices, groups, shards,
    x_hbm, order_s, meta_v, sharp_ref, gain_ref, bias_ref, attribute_ref, feeder_ref, project_ref,
    offset_row_ref, question_ref, lookup_ref, content_ref, emit_ref, emit_bias_ref,
    gain2_ref, bias2_ref, entry_bias_ref, exit_bias_ref, entry_hbm, exit_hbm,
    res_hbm, meta_in,
    x_v, xf, stage, send_v, recv_v, res, share_v, entry_ref, exit_ref,
    sharp_v, sharp_in, w_ref, expand_ref, offset_ref, scale_ref, numer, total,
    part_out, part_in, mine, all_in, sums_v, blend,
    local_sem, out_sem, row_send, row_recv, meta_send, meta_recv, sharp_send, sharp_recv,
    part_send, part_recv, all_send, all_recv,
):
    devices = groups * shards
    rows, width = x_v.shape
    per_pair = rows // devices
    tile = rows // STEPS
    blocks = devices // STEPS
    sum_tile = rows // SUM_STEPS
    columns = expand_ref.shape[0]
    own = sharp_ref.shape[1]
    my_head, my_pts = lax.axis_index("head"), lax.axis_index("pts")
    me = my_head * shards + my_pts

    unit = devices // UNITS
    heads = [flip(my_head, jnp.int32(at), groups) for at in range(groups)]
    shard_ids = [flip(my_pts, jnp.int32(at), shards) for at in range(shards)]

    def peer(slot):
        return heads[slot % groups], shard_ids[mirror(slot // groups, shards)]

    def flat(slot):
        head, pts = peer(slot)
        return head * shards + pts

    def each_peer(step):
        for slot in range(1, devices):
            step(slot)

    def loop(low, high, step):
        def run(at, carry):
            step(at)
            return carry
        lax.fori_loop(low, high, run, 0)

    barrier = pltpu.get_barrier_semaphore()
    load = pltpu.make_async_copy(x_hbm, x_v, local_sem.at[0])
    load.start()
    each_peer(lambda slot: pl.semaphore_signal(
        barrier, 1, device_id=peer(slot), device_id_type=MESH
    ))
    entry_load = pltpu.make_async_copy(entry_hbm, entry_ref, local_sem.at[1])
    exit_load = pltpu.make_async_copy(exit_hbm, exit_ref, local_sem.at[2])
    entry_load.start()
    exit_load.start()

    sharp_v[...] = jnp.zeros_like(sharp_v)
    sharp_v[:, :own] = sharp_ref[...]
    sharp_in[my_head] = sharp_v[...]

    w_ref[:width] = attribute_ref[...].astype(F32).T.astype(BF16)
    w_ref[width:] = feeder_ref[...].astype(F32).T.astype(BF16)
    repeated = jnp.concatenate([project_ref[...].astype(F32).T] * (columns // slices), axis=0)
    lane = lax.broadcasted_iota(I32, (DH, width), 1) % DH
    pick = (lane == lax.broadcasted_iota(I32, (DH, width), 0)).astype(F32).astype(BF16)
    filled = jnp.dot(repeated.astype(BF16), pick, preferred_element_type=F32)
    expand_ref[...] = jnp.where(same_head(filled.shape, slices, DH), filled, 0.0).astype(BF16)
    row = lax.broadcasted_iota(I32, (columns, slices), 0) % slices
    match = row == lax.broadcasted_iota(I32, (columns, slices), 1)
    offset_ref[...] = jnp.sum(jnp.where(match, offset_row_ref[...], 0.0), axis=1, keepdims=True)
    numer[...] = jnp.zeros_like(numer)
    total[...] = jnp.zeros_like(total)

    load.wait()

    def widen(at):
        part = x_v[pl.ds(pl.multiple_of(at * tile, tile), tile), :].astype(F32)
        xf[pl.ds(at * 2 * tile, tile, stride=2), :] = part[:, :LANES]
        xf[pl.ds(at * 2 * tile + 1, tile, stride=2), :] = part[:, LANES:]

    def collect(at):
        for way in range(blocks):
            def take(k, carry):
                put = pl.multiple_of(2 * (way * per_pair + k), 2)
                stage[pl.ds(put, 2), :] = xf[pl.ds(order_s[at * blocks + way, k], 2), :]
                return carry
            lax.fori_loop(0, per_pair, take, 0, unroll=True)
        span = slice(at * tile, (at + 1) * tile)
        send_v[span, :LANES] = stage[pl.ds(0, tile, stride=2), :].astype(BF16)
        send_v[span, LANES:] = stage[pl.ds(1, tile, stride=2), :].astype(BF16)

    loop(0, STEPS, widen)
    for at in range(STEPS // 2):
        collect(at)
    pl.semaphore_wait(barrier, devices - 1)

    def sharp_copy(step):
        return pltpu.make_async_remote_copy(
            sharp_v, sharp_in.at[my_head], sharp_send.at[step], sharp_recv.at[step],
            device_id=(heads[step], my_pts), device_id_type=MESH,
        )

    def meta_copy(slot):
        return pltpu.make_async_remote_copy(
            meta_v.at[slot], meta_in.at[slot], meta_send.at[slot], meta_recv.at[slot],
            device_id=peer(slot), device_id_type=MESH,
        )

    def row_copy(slot, goal):
        span = pl.ds(pl.multiple_of(slot * per_pair, per_pair), per_pair)
        return pltpu.make_async_remote_copy(
            send_v.at[span], recv_v.at[span], row_send.at[slot], row_recv.at[slot],
            device_id=goal, device_id_type=MESH,
        )

    def far_goal(slot):
        shard = mirror(lax.div(slot, groups), shards)
        return flip(my_head, lax.rem(slot, groups), groups), flip(my_pts, shard, shards)

    def send_units(low, high):
        for slot in range(max(low * unit, 1), high * unit):
            row_copy(slot, peer(slot)).start()

    def part_copy(slot):
        return pltpu.make_async_remote_copy(
            part_out.at[flat(slot)], part_in.at[slot], part_send.at[slot], part_recv.at[slot],
            device_id=peer(slot), device_id_type=MESH,
        )

    def all_copy(slot):
        return pltpu.make_async_remote_copy(
            mine, all_in.at[me], all_send.at[slot], all_recv.at[slot],
            device_id=peer(slot), device_id_type=MESH,
        )

    for step in range(1, groups):
        sharp_copy(step).start()
    send_units(0, FIRST)
    for at in range(STEPS // 2, STEPS):
        collect(at)
    for step in range(1, groups):
        sharp_copy(step).wait()
    per_group = own * slices
    for group in range(groups):
        lane = lax.broadcasted_iota(I32, (per_group, LANES), 1)
        member = lax.broadcasted_iota(I32, (per_group, LANES), 0) // slices
        sharp = jnp.sum(jnp.where(lane == member, sharp_in[group], 0.0), axis=1, keepdims=True)
        scale_ref[group * per_group : (group + 1) * per_group] = LOG2E / sharp

    def sums_step(at):
        @pl.when(lax.rem(at * (EARLY - FIRST), SUM_STEPS) < EARLY - FIRST)
        def _():
            at_unit = FIRST + lax.div(at * (EARLY - FIRST), SUM_STEPS)
            for way in range(unit):
                slot = at_unit * unit + way
                row_copy(slot, far_goal(slot)).start()

        span = pl.ds(pl.multiple_of(at * sum_tile, sum_tile), sum_tile)
        normed = norm_rows(x_v[span, :].astype(F32), gain_ref[...], bias_ref[...])
        both = lax.dot_general(w_ref[...], normed, NT, preferred_element_type=F32).astype(BF16)
        share = slice_weights(
            both[width:], expand_ref[...], offset_ref[...], scale_ref[...], slices
        )
        numer[...] += lax.dot_general(
            both[:width], share.astype(BF16), NT, preferred_element_type=F32
        )
        part = share[:, :LANES]
        for low in range(LANES, sum_tile, LANES):
            part += share[:, low : low + LANES]
        total[...] += part

    loop(0, SUM_STEPS, sums_step)

    kept = jnp.where(same_head(numer.shape, DH, slices), numer[...], 0.0)
    sums_v[:DH] = jnp.sum(kept.reshape(-1, DH, columns), axis=0)
    sums_v[DH:] = lax.dot_general(
        jnp.ones((8, LANES), F32), total[...], NT, precision=HIGHEST, preferred_element_type=F32
    )
    per_row = columns // LANES
    depth = part_out.shape[1]
    places = [
        (at // per_row, at % per_row * LANES, at // depth, at % depth)
        for at in range((DH + 1) * per_row)
    ]
    part_out[...] = jnp.zeros_like(part_out)
    for line, low, piece, inner in places:
        part_out[piece, inner : inner + 1, :] = sums_v[line : line + 1, low : low + LANES]
    each_peer(lambda slot: part_copy(slot).start())
    part_in[0] = part_out[me]
    send_units(EARLY, EARLY + MID)
    each_peer(lambda slot: meta_copy(slot).start())
    meta_in[0] = meta_v[0]
    recv_v[:per_pair] = send_v[:per_pair]

    def wait_rows(at):
        for way in range(blocks):
            slot = at * blocks + way

            @pl.when(slot > 0)
            def _():
                row_copy(slot, (my_head, my_pts)).wait_recv()

    def weigh(at):
        x = recv_v[pl.ds(pl.multiple_of(at * tile, tile), tile), :].astype(F32)
        normed = norm_rows(x, gain_ref[...], bias_ref[...])
        feeder = lax.dot_general(
            w_ref[width:], normed, NT, preferred_element_type=F32
        ).astype(BF16)
        share = slice_weights(feeder, expand_ref[...], offset_ref[...], scale_ref[...], slices)
        return share.astype(BF16)

    def weigh_ahead(at):
        wait_rows(at)
        share_v[at] = weigh(at)

    loop(0, AHEAD[0], weigh_ahead)

    each_peer(lambda slot: part_copy(slot).wait())
    mine[...] = jnp.sum(part_in[...], axis=0)
    each_peer(lambda slot: all_copy(slot).start())
    send_units(EARLY + MID, UNITS)
    all_in[me] = mine[...]
    loop(AHEAD[0], AHEAD[1], weigh_ahead)
    each_peer(lambda slot: all_copy(slot).wait())
    for line, low, piece, inner in places:
        sums_v[line : line + 1, low : low + LANES] = all_in[piece, inner : inner + 1, :]

    stok = sums_v[:DH] / (sums_v[DH : DH + 1] + 1e-05)
    query, key, value = (
        jnp.dot(m[...].T, stok, precision=HIGHEST, preferred_element_type=F32)
        for m in (question_ref, lookup_ref, content_ref)
    )
    scores = jnp.dot(key.T, query, precision=HIGHEST, preferred_element_type=F32)
    scores = scores * (1.0 / math.sqrt(DH))
    mask = same_head(scores.shape, slices, slices)
    scores = jnp.where(mask, scores, -jnp.inf)
    powers = jnp.exp(scores - jnp.max(scores, axis=0, keepdims=True))
    attention = powers / jnp.sum(powers, axis=0, keepdims=True)
    sout = jnp.dot(value, attention, precision=HIGHEST, preferred_element_type=F32)
    spread = jnp.concatenate([sout] * (width // DH), axis=0)
    blend[...] = jnp.where(same_head(blend.shape, DH, slices), spread, 0.0).astype(BF16)
    entry_load.wait()
    exit_load.wait()

    def finish(at, share):
        x = recv_v[pl.ds(pl.multiple_of(at * tile, tile), tile), :].astype(F32)
        mixed = jnp.dot(blend[...], share, preferred_element_type=F32)
        y = (
            x
            + jnp.dot(mixed.T.astype(BF16), emit_ref[...], preferred_element_type=F32)
            + emit_bias_ref[...]
        )
        z = norm_rows(y, gain2_ref[...], bias2_ref[...])
        result = y + exit_bias_ref[...]
        for low in range(0, entry_ref.shape[1], width):
            h = jnp.dot(z, entry_ref[:, low : low + width], preferred_element_type=F32)
            g = exact_gelu(h + entry_bias_ref[:, low : low + width]).astype(BF16)
            result += jnp.dot(g, exit_ref[low : low + width], preferred_element_type=F32)
        res[pl.ds(at * 2 * tile, tile, stride=2), :] = result[:, :LANES]
        res[pl.ds(at * 2 * tile + 1, tile, stride=2), :] = result[:, LANES:]
        out_copy(at).start()

    def out_copy(at):
        span = pl.ds(pl.multiple_of(at * 2 * tile, 2 * tile), 2 * tile)
        return pltpu.make_async_copy(res.at[span], res_hbm.at[span], out_sem.at[at])

    loop(0, AHEAD[1], lambda at: finish(at, share_v[at]))

    def rows_step(at):
        wait_rows(at)
        finish(at, weigh(at))

    loop(AHEAD[1], STEPS, rows_step)
    each_peer(lambda slot: meta_copy(slot).wait())
    each_peer(lambda slot: row_copy(slot, peer(slot)).wait_send())
    loop(0, STEPS, lambda at: out_copy(at).wait())


def serve_kernel(spot_s, res_hbm, out_hbm, res, placed, out_v, in_sem, out_sem):
    rows = out_v.shape[0]
    tile = rows // STEPS
    part = rows // PARTS
    blocks = spot_s.shape[0] // STEPS
    per_pair = tile // blocks

    def res_copy(at):
        span = pl.ds(pl.multiple_of(at * 2 * tile, 2 * tile), 2 * tile)
        return pltpu.make_async_copy(res_hbm.at[span], res.at[span], in_sem.at[at])

    def out_copy(at):
        span = pl.ds(pl.multiple_of(at * part, part), part)
        return pltpu.make_async_copy(out_v.at[span], out_hbm.at[span], out_sem.at[at])

    for at in range(STEPS):
        res_copy(at).start()

    for at in range(STEPS):
        res_copy(at).wait()
        for slot in range(at * blocks, (at + 1) * blocks):
            def put(k, carry):
                spot = pl.multiple_of(spot_s[slot, 0, k], 2)
                low = pl.multiple_of(2 * (slot * per_pair + k), 2)
                placed[pl.ds(spot, 2), :] = res[pl.ds(low, 2), :]
                return carry
            lax.fori_loop(0, per_pair, put, 0, unroll=True)

    def narrow(at, carry):
        first = at * 2 * part
        span = pl.ds(pl.multiple_of(at * part, part), part)
        out_v[span, :LANES] = placed[pl.ds(first, part, stride=2), :].astype(BF16)
        out_v[span, LANES:] = placed[pl.ds(first + 1, part, stride=2), :].astype(BF16)
        out_copy(at).start()
        return carry

    lax.fori_loop(0, PARTS, narrow, 0)
    for at in range(PARTS):
        out_copy(at).wait()


def body(
    layer_inputs_trainorder,
    inference_placement,
    initial_layernorm_gain,
    initial_layernorm_offset,
    attribute_projection,
    assignment_feeder_projection,
    partition_projection,
    partition_offset,
    softmax_sharpness,
    partition_question_map,
    partition_lookup_map,
    partition_content_map,
    emitted_projection,
    emitted_offset,
    latter_layernorm_gain,
    latter_layernorm_offset,
    perceptron_entry_map,
    perceptron_entry_offset,
    perceptron_exit_map,
    perceptron_exit_offset,
):
    groups = lax.axis_size("head")
    shards = lax.axis_size("pts")
    devices = groups * shards
    rows, width = layer_inputs_trainorder.shape
    per_pair = rows // devices
    slices = partition_projection.shape[1]
    columns = softmax_sharpness.shape[0] * groups * slices
    wide = -(-per_pair // LANES) * LANES
    tile = rows // STEPS
    depth = -(-(DH + 1) * (columns // LANES) // devices)
    order, spots = pl.pallas_call(
        functools.partial(index_kernel, groups, shards, rows),
        out_shape=(
            jax.ShapeDtypeStruct((devices, per_pair), I32),
            jax.ShapeDtypeStruct((devices, 1, wide), I32),
        ),
        scratch_shapes=[pltpu.VMEM((1, rows), I32)] * 3,
    )(inference_placement[None])
    operands = (
        order, spots, softmax_sharpness[None], initial_layernorm_gain[None],
        initial_layernorm_offset[None], attribute_projection, assignment_feeder_projection,
        partition_projection, partition_offset[None], partition_question_map,
        partition_lookup_map, partition_content_map, emitted_projection, emitted_offset[None],
        latter_layernorm_gain[None], latter_layernorm_offset[None],
        perceptron_entry_offset[None], perceptron_exit_offset[None], perceptron_entry_map,
        perceptron_exit_map,
    )
    dma = pltpu.SemaphoreType.DMA
    scratch = [
        pltpu.VMEM((rows, width), BF16),
        pltpu.VMEM((2 * rows, LANES), F32),
        pltpu.VMEM((2 * tile, LANES), F32),
        pltpu.VMEM((rows, width), BF16),
        pltpu.VMEM((rows, width), BF16),
        pltpu.VMEM((2 * rows, LANES), F32),
        pltpu.VMEM((AHEAD[1], columns, tile), BF16),
        pltpu.VMEM(perceptron_entry_map.shape, BF16),
        pltpu.VMEM(perceptron_exit_map.shape, BF16),
        pltpu.VMEM((1, LANES), F32),
        pltpu.VMEM((groups, 1, LANES), F32),
        pltpu.VMEM((2 * width, width), BF16),
        pltpu.VMEM((columns, width), BF16),
        pltpu.VMEM((columns, 1), F32),
        pltpu.VMEM((columns, 1), F32),
        pltpu.VMEM((width, columns), F32),
        pltpu.VMEM((columns, LANES), F32),
        pltpu.VMEM((devices, depth, LANES), F32),
        pltpu.VMEM((devices, depth, LANES), F32),
        pltpu.VMEM((depth, LANES), F32),
        pltpu.VMEM((devices, depth, LANES), F32),
        pltpu.VMEM((DH + 8, columns), F32),
        pltpu.VMEM((width, columns), BF16),
        dma((3,)),
        dma((STEPS,)),
        dma((devices,)),
        dma((devices,)),
        dma((devices,)),
        dma((devices,)),
        dma((groups,)),
        dma((groups,)),
        dma((devices,)),
        dma((devices,)),
        dma((devices,)),
        dma((devices,)),
    ]
    in_vmem = pl.BlockSpec(memory_space=pltpu.VMEM)
    res, arrived = pl.pallas_call(
        functools.partial(fused_kernel, slices, groups, shards),
        out_shape=(
            jax.ShapeDtypeStruct((2 * rows, LANES), F32),
            jax.ShapeDtypeStruct((devices, 1, wide), I32),
        ),
        in_specs=[pl.BlockSpec(memory_space=pl.ANY), pl.BlockSpec(memory_space=pltpu.SMEM)]
        + [in_vmem] * (len(operands) - 3)
        + [pl.BlockSpec(memory_space=pl.ANY)] * 2,
        out_specs=(pl.BlockSpec(memory_space=pl.ANY), in_vmem),
        scratch_shapes=scratch,
        compiler_params=pltpu.CompilerParams(
            collective_id=0, has_side_effects=True, vmem_limit_bytes=60 * 2**20
        ),
        cost_estimate=pl.CostEstimate(
            flops=rows * width * columns * 24, bytes_accessed=rows * width * 8,
            transcendentals=rows * columns * 4,
        ),
    )(layer_inputs_trainorder, *operands)
    anywhere = pl.BlockSpec(memory_space=pl.ANY)
    out = pl.pallas_call(
        serve_kernel,
        in_specs=[pl.BlockSpec(memory_space=pltpu.SMEM), anywhere],
        out_specs=anywhere,
        out_shape=jax.ShapeDtypeStruct((rows, width), BF16),
        scratch_shapes=[
            pltpu.VMEM((2 * rows, LANES), F32),
            pltpu.VMEM((2 * rows, LANES), F32),
            pltpu.VMEM((rows, width), BF16),
            dma((STEPS,)),
            dma((PARTS,)),
        ],
    )(arrived, res)
    return out[None]


def solution(mesh):
    placed = (
        P(("head", "pts"), None),
        P(("head", "pts")),
        P(),
        P(),
        P(),
        P(),
        P(),
        P(),
        P("head"),
        P(),
        P(),
        P(),
        P(),
        P(),
        P(),
        P(),
        P(),
        P(),
        P(),
        P(),
    )
    return jax.shard_map(
        body, mesh=mesh, in_specs=placed, out_specs=P("pts", "head", None), check_vma=False
    )
```
